32 devices in a mesh: tm: 8 (over z, y), series: 4 (over x, core).
Axes of the slice: x: 2, y: 2, z: 4, core: 2. Of those that a mesh axis runs over, the one named last changes fastest.
Arguments:
- returns: float32 [2048, 8192], P('tm', 'series'), may hold values from -40 to 40
- sector: int32 [8192], P('series'), may hold values from 0 to 511, as said below
Outputs:
- shrunk_variance: float32 [2048, 8192], P('tm', 'series')
The draws below stay inside these ranges and needn't reach their ends.
Inputs may be any that keep to these rules, and one draw needn't show every extreme that they name: `sector`: sectors differ widely in size; some sectors may hold no series.
All inputs are finite; a program needn't handle non-finite values.
Results may differ from the reference program's by a relative error of at most 0.0003.
Values sent between devices are 32-bit elements; how exact they have to be, the bound alone decides.
No kernel may reach another device: no remote copies, remote signals or barrier semaphores. Data moves between devices by JAX's collectives and lax.ppermute only.
A program may use at most 64 MiB of HBM per device.

```python
import jax
import jax.numpy as jnp
from jax import lax

T_DEV = 256
W = 64
SECTORS = 512
STEPS = 2048
SERIES = 8192
N_TM = 8


def sector_labels(key):
    base = jax.random.fold_in(key, 1013)
    first = jax.random.randint(jax.random.fold_in(base, 1), (SERIES,), 0, SECTORS)
    second = jax.random.randint(jax.random.fold_in(base, 2), (SERIES,), 0, SECTORS)
    raw = first * second // SECTORS
    order = jax.random.permutation(jax.random.fold_in(base, 3), SECTORS)
    return order[raw].astype(jnp.int32)


def draw_sector(key, part):
    return sector_labels(key)


def draw_returns(key, part):
    labels = sector_labels(key)
    base = jax.random.fold_in(key, 2027)
    common = jax.random.normal(jax.random.fold_in(base, 1), (STEPS, SECTORS), jnp.float32)
    loading = jax.random.uniform(jax.random.fold_in(base, 2), (SERIES,), jnp.float32, 0.5, 1.5)
    volatility = jnp.exp(jax.random.uniform(jax.random.fold_in(base, 3), (SERIES,), jnp.float32, jnp.log(0.3), jnp.log(1.5)))
    position = jnp.arange(STEPS, dtype=jnp.float32) / STEPS
    noise = jax.random.normal(jax.random.fold_in(base, 4), (STEPS, SERIES), jnp.float32)
    trend = 1.0 + 2.0 * position
    values = trend[:, None] * (loading[None, :] * common[:, labels] + volatility[None, :] * noise)
    return jnp.clip(values, -40.0, 40.0).astype(jnp.float32)


def setup_inputs(seed: int = 0) -> dict:
    streams_of = jax.random.split(jax.random.key(seed), 3)
    return {
        "returns": draw_returns(jax.random.fold_in(streams_of[2], 71), 0),
        "sector": draw_sector(jax.random.fold_in(streams_of[2], 71), 0),
    }


ridge_rate = 0.05
shrink_weight = 0.3
highest = lax.Precision.HIGHEST


def sector_table(sector):
    labels = jnp.arange(SECTORS, dtype=jnp.int32)
    return (sector[:, None] == labels[None, :]).astype(jnp.float32)


def band_matrix(rows):
    row_pos = jnp.arange(rows, dtype=jnp.int32)[:, None]
    col_pos = jnp.arange(rows + W - 1, dtype=jnp.int32)[None, :]
    return ((col_pos >= row_pos) & (col_pos < row_pos + W)).astype(jnp.float32)


def window_variance(ext_returns, ext_factor, first_step):
    rows = ext_returns.shape[0] - (W - 1)
    series_width = ext_returns.shape[1]
    stacked = jnp.concatenate([ext_returns, ext_factor, ext_returns * ext_returns,
                               ext_factor * ext_factor, ext_returns * ext_factor], axis=1)
    moments = jnp.dot(band_matrix(rows), stacked, precision=highest, preferred_element_type=jnp.float32)
    sum_ret = moments[:, :series_width]
    sum_fac = moments[:, series_width:2 * series_width]
    sum_rr = moments[:, 2 * series_width:3 * series_width]
    sum_ff = moments[:, 3 * series_width:4 * series_width]
    sum_rf = moments[:, 4 * series_width:]
    steps_seen = jnp.minimum(first_step + jnp.arange(rows, dtype=jnp.int32) + 1, W).astype(jnp.float32)[:, None]
    centred_rr = sum_rr - sum_ret * sum_ret / steps_seen
    centred_ff = sum_ff - sum_fac * sum_fac / steps_seen
    centred_rf = sum_rf - sum_ret * sum_fac / steps_seen
    return (centred_rr - centred_rf * centred_rf / (centred_ff + ridge_rate * steps_seen)) / steps_seen


def reference(returns, sector):
    table = sector_table(sector)
    sums = jnp.dot(returns, table, precision=highest, preferred_element_type=jnp.float32)
    counts = jnp.sum(table, axis=0)
    means = sums / jnp.maximum(counts, 1.0)[None, :]
    factor = jnp.dot(means, table.T, precision=highest, preferred_element_type=jnp.float32)
    zeros = jnp.zeros((W - 1, SERIES), jnp.float32)
    padded_ret = jnp.concatenate([zeros, returns], axis=0)
    padded_fac = jnp.concatenate([zeros, factor], axis=0)

    def block(block_index):
        start = (block_index * T_DEV).astype(jnp.int32)
        ext_returns = lax.dynamic_slice_in_dim(padded_ret, start, T_DEV + W - 1, 0)
        ext_factor = lax.dynamic_slice_in_dim(padded_fac, start, T_DEV + W - 1, 0)
        return window_variance(ext_returns, ext_factor, start)

    variance = lax.map(block, jnp.arange(N_TM, dtype=jnp.int32)).reshape(STEPS, SERIES)
    totals = jnp.dot(jnp.sum(variance, axis=0)[None, :], table, precision=highest, preferred_element_type=jnp.float32)[0]
    sector_mean = totals / (STEPS * jnp.maximum(counts, 1.0))
    pooled = jnp.dot(sector_mean[None, :], table.T, precision=highest, preferred_element_type=jnp.float32)
    return (1.0 - shrink_weight) * variance + shrink_weight * pooled
```

```python
import functools

import jax
import jax.numpy as jnp
from jax import lax
from jax.experimental import pallas as pl
from jax.experimental.pallas import tpu as pltpu
from jax.sharding import PartitionSpec as P

W = 64
SECTORS = 512
HALF = SECTORS // 2
LANES = 128

ridge_rate = 0.05
shrink_weight = 0.3

f32 = jnp.float32
bf16 = jnp.bfloat16
MIB = 1024 * 1024


def dot_nn(a, b):
    return lax.dot_general(a, b, (((1,), (0,)), ((), ())), preferred_element_type=f32)


def dot_nt(a, b):
    return lax.dot_general(a, b, (((1,), (1,)), ((), ())), preferred_element_type=f32)


def split2(x):
    hi = x.astype(bf16)
    return hi, (x - hi.astype(f32)).astype(bf16)


def split3_rows(x):
    hi = x.astype(bf16).astype(f32)
    rest = x - hi
    mid = rest.astype(bf16).astype(f32)
    low = rest - mid
    row = lax.broadcasted_iota(jnp.int32, (16, x.shape[1]), 0)
    return jnp.where(row == 0, hi, jnp.where(row == 1, mid, jnp.where(row == 2, low, 0.0))).astype(bf16)


def window(x):
    size = 1
    while size < W:
        x = x + pltpu.roll(x, size, 0)
        size *= 2
    return x[W:]


def sums_kernel(core_ref, ret_ref, sec_ref, keep_ref, send_ref, table_ref, tail_ref, hi_ref, lo_ref):
    rows = ret_ref.shape[0]
    core = core_ref[0]
    label = lax.broadcasted_iota(jnp.int32, table_ref.shape, 0)
    label = (label + core * HALF) & (SECTORS - 1)
    table_ref[...] = jnp.where(label == sec_ref[...], 1.0, 0.0).astype(bf16)
    value = ret_ref[...]
    hi, lo = split2(value)
    hi_ref[:rows] = hi
    lo_ref[:rows] = lo
    hi_ref[rows:] = jnp.ones_like(hi_ref[rows:])
    lo_ref[rows:] = jnp.zeros_like(lo_ref[rows:])
    tail_ref[...] = ret_ref[rows - W :]
    acc = dot_nt(hi_ref[...], table_ref[...]) + dot_nt(lo_ref[...], table_ref[...])
    keep_ref[...] = acc[: rows + 8, :HALF]
    send_ref[...] = acc[: rows + 8, HALF:]


def sector_sums(core, returns, sector):
    rows, width = returns.shape
    half = jax.ShapeDtypeStruct((rows + 8, HALF), f32)
    return pl.pallas_call(
        sums_kernel,
        out_shape=(
            half,
            half,
            jax.ShapeDtypeStruct((SECTORS, width), bf16),
            jax.ShapeDtypeStruct((W, width), f32),
        ),
        in_specs=[
            pl.BlockSpec(memory_space=pltpu.SMEM),
            pl.BlockSpec(memory_space=pltpu.VMEM),
            pl.BlockSpec(memory_space=pltpu.VMEM),
        ],
        out_specs=[pl.BlockSpec(memory_space=pltpu.VMEM)] * 4,
        scratch_shapes=[pltpu.VMEM((rows + 16, width), bf16)] * 2,
        compiler_params=pltpu.CompilerParams(vmem_limit_bytes=24 * MIB),
        cost_estimate=pl.CostEstimate(
            flops=4 * rows * width * SECTORS, bytes_accessed=8 * rows * width, transcendentals=0
        ),
        name="sector_sums",
    )(core, returns, sector)


def variance_kernel(
    info_ref, own_ref, other_ref, hown_ref, hother_ref, halo_ref, ret_ref, table_ref,
    var_ref, totals_ref, hi_ref, lo_ref, steps_ref, acc_ref,
):
    rows = ret_ref.shape[0]
    ext = rows + W
    step = pl.program_id(0)
    core, first_step = info_ref[0], info_ref[1]

    @pl.when(step == 0)
    def _():
        position = lax.broadcasted_iota(jnp.int32, (rows, LANES), 0) + (first_step + 1)
        inv = 1.0 / jnp.minimum(position, W).astype(f32)
        steps_ref[...] = inv
        for tile in range(SECTORS // LANES):
            here, prior = (own_ref, hown_ref) if tile < HALF // LANES else (other_ref, hother_ref)
            cols = pl.ds((tile * LANES) % HALF, LANES)
            count = jnp.maximum(here[rows : rows + 1, cols], 1.0)
            mean = jnp.concatenate([prior[:, cols], here[:rows, cols]], axis=0) / count
            mean_f = window(mean) * inv
            cff = window(mean * mean) * inv - mean_f * mean_f
            gain = 1.0 / (cff + ridge_rate)
            out = pl.ds(tile * LANES, LANES)
            for start, part in ((0, mean), (ext, mean_f), (ext + rows, gain)):
                hi, lo = split2(part)
                hi_ref[start : start + part.shape[0], out] = hi
                lo_ref[start : start + part.shape[0], out] = lo
        acc_ref[...] = jnp.zeros_like(acc_ref)

    inv = steps_ref[...]
    spread = dot_nn(hi_ref[...], table_ref[...]) + dot_nn(lo_ref[...], table_ref[...])
    column_sums = []
    for tile in range(ret_ref.shape[1] // LANES):
        cols = slice(tile * LANES, (tile + 1) * LANES)
        ret = jnp.concatenate([halo_ref[:, cols], ret_ref[:, cols]], axis=0)
        factor = spread[:ext, cols]
        mean_f = spread[ext : ext + rows, cols]
        gain = spread[ext + rows :, cols]
        mean_r = window(ret) * inv
        crr = window(ret * ret) * inv - mean_r * mean_r
        crf = window(ret * factor) * inv - mean_r * mean_f
        variance = crr - crf * crf * gain
        var_ref[:, cols] = (1.0 - shrink_weight) * variance
        column_sums.append(jnp.sum(variance, axis=0, keepdims=True))
    acc_ref[...] += dot_nt(split3_rows(jnp.concatenate(column_sums, axis=1)), table_ref[...])

    @pl.when(step == pl.num_programs(0) - 1)
    def _():
        total = jnp.sum(acc_ref[...], axis=0, keepdims=True)
        swapped = jnp.concatenate([total[:, HALF:], total[:, :HALF]], axis=1)
        total = jnp.where(core == 0, total, swapped)
        totals_ref[...] = jnp.broadcast_to(total, totals_ref.shape)


def window_variance(info, own, other, hown, hother, halo, returns, table, devices):
    rows, width = returns.shape
    block = 2 * LANES
    fixed = lambda a: pl.BlockSpec(a.shape, lambda i: (0, 0))
    return pl.pallas_call(
        variance_kernel,
        grid=(width // block,),
        out_shape=(
            jax.ShapeDtypeStruct((rows, width), f32),
            jax.ShapeDtypeStruct((devices, SECTORS), f32),
        ),
        in_specs=[
            pl.BlockSpec(memory_space=pltpu.SMEM),
            fixed(own), fixed(other), fixed(hown), fixed(hother),
            pl.BlockSpec((W, block), lambda i: (0, i)),
            pl.BlockSpec((rows, block), lambda i: (0, i)),
            pl.BlockSpec((SECTORS, block), lambda i: (0, i)),
        ],
        out_specs=[
            pl.BlockSpec((rows, block), lambda i: (0, i)),
            pl.BlockSpec((devices, SECTORS), lambda i: (0, 0)),
        ],
        scratch_shapes=[
            pltpu.VMEM((3 * rows + W, SECTORS), bf16),
            pltpu.VMEM((3 * rows + W, SECTORS), bf16),
            pltpu.VMEM((rows, LANES), f32),
            pltpu.VMEM((16, SECTORS), f32),
        ],
        compiler_params=pltpu.CompilerParams(vmem_limit_bytes=24 * MIB),
        cost_estimate=pl.CostEstimate(
            flops=12 * rows * width * SECTORS, bytes_accessed=12 * rows * width, transcendentals=0
        ),
        name="window_variance",
    )(info, own, other, hown, hother, halo, returns, table)


def shrink_kernel(all_steps, core_ref, parts_ref, cown_ref, cother_ref, table_ref, var_ref, out_ref, pooled_ref):
    @pl.when(pl.program_id(0) == 0)
    def _():
        total = jnp.sum(parts_ref[...], axis=0, keepdims=True)
        swapped = jnp.concatenate([total[:, HALF:], total[:, :HALF]], axis=1)
        total = jnp.where(core_ref[0] == 0, total, swapped)
        count = jnp.concatenate([cown_ref[0:1], cother_ref[0:1]], axis=1)
        mean = total / (all_steps * jnp.maximum(count, 1.0))
        spread = dot_nn(split3_rows(shrink_weight * mean), table_ref[...])
        pooled_ref[...] = jnp.broadcast_to(
            jnp.sum(spread, axis=0, keepdims=True), pooled_ref.shape
        )

    out_ref[...] = var_ref[...] + pooled_ref[0:1]


def shrink(all_steps, core, parts, own, other, table, variance):
    rows, width = variance.shape
    block = rows // 4
    tail = pl.BlockSpec((8, HALF), lambda i: (rows // 8, 0))
    return pl.pallas_call(
        functools.partial(shrink_kernel, float(all_steps)),
        grid=(rows // block,),
        out_shape=jax.ShapeDtypeStruct((rows, width), f32),
        in_specs=[
            pl.BlockSpec(memory_space=pltpu.SMEM),
            pl.BlockSpec(parts.shape, lambda i: (0, 0)),
            tail,
            tail,
            pl.BlockSpec(table.shape, lambda i: (0, 0)),
            pl.BlockSpec((block, width), lambda i: (i, 0)),
        ],
        out_specs=pl.BlockSpec((block, width), lambda i: (i, 0)),
        scratch_shapes=[pltpu.VMEM((8, width), f32)],
        compiler_params=pltpu.CompilerParams(vmem_limit_bytes=24 * MIB),
        cost_estimate=pl.CostEstimate(
            flops=2 * rows * width, bytes_accessed=8 * rows * width, transcendentals=0
        ),
        name="shrink",
    )(core, parts, own, other, table, variance)


def swap(value, axis, bit):
    return lax.ppermute(value, axis, [(i, i ^ bit) for i in range(lax.axis_size(axis))])


def ahead(value, axis):
    return lax.ppermute(value, axis, [(i, i + 1) for i in range(lax.axis_size(axis) - 1)])


def across(value, axis):
    bit = 2
    while bit < lax.axis_size(axis):
        value = value + swap(value, axis, bit)
        bit *= 2
    return value


def local(returns, sector):
    rows, width = returns.shape
    n_time, n_series = lax.axis_size("tm"), lax.axis_size("series")
    core = (lax.axis_index("series") % 2).astype(jnp.int32)
    first_step = (lax.axis_index("tm") * rows).astype(jnp.int32)
    info = jnp.stack([core, first_step])
    keep, send, table, tail = sector_sums(info, returns, sector[None, :])
    part = keep + swap(send, "series", 1)
    part_tail = ahead(part[rows - W : rows], "tm")
    halo = ahead(tail, "tm")
    own = across(part, "series")
    own_tail = across(part_tail, "series")
    other = swap(own, "series", 1)
    other_tail = swap(own_tail, "series", 1)
    variance, totals = window_variance(
        info, own, other, own_tail, other_tail, halo, returns, table, n_time * n_series
    )
    parts = lax.all_to_all(totals, ("tm", "series"), 0, 0)
    return shrink(n_time * rows, info, parts, own, other, table, variance)


def solution(mesh):
    placed = (P("tm", "series"), P("series"))
    return jax.shard_map(
        local, mesh=mesh, in_specs=placed, out_specs=P("tm", "series"), check_vma=False
    )
```

```python
import functools

import jax
import jax.numpy as jnp
from jax import lax
from jax.experimental import pallas as pl
from jax.experimental.pallas import tpu as pltpu
from jax.sharding import PartitionSpec as P


W = 64
SECTORS = 512
HALF = SECTORS // 2
LANES = 128

ridge_rate = 0.05
shrink_weight = 0.3

f32 = jnp.float32
bf16 = jnp.bfloat16
MIB = 1024 * 1024


def dot_nn(a, b):
    return lax.dot_general(a, b, (((1,), (0,)), ((), ())), preferred_element_type=f32)


def dot_nt(a, b):
    return lax.dot_general(a, b, (((1,), (1,)), ((), ())), preferred_element_type=f32)


def split2(x):
    hi = x.astype(bf16)
    return hi, (x - hi.astype(f32)).astype(bf16)


def split3_rows(x):
    hi = x.astype(bf16).astype(f32)
    rest = x - hi
    mid = rest.astype(bf16).astype(f32)
    low = rest - mid
    row = lax.broadcasted_iota(jnp.int32, (16, x.shape[1]), 0)
    return jnp.where(row == 0, hi, jnp.where(row == 1, mid, jnp.where(row == 2, low, 0.0))).astype(bf16)


def sums_kernel(core_ref, ret_ref, sec_ref, keep_ref, send_ref, table_ref, tail_ref, hi_ref, lo_ref):
    rows = ret_ref.shape[0]
    core = core_ref[0]
    label = lax.broadcasted_iota(jnp.int32, table_ref.shape, 0)
    label = (label + core * HALF) & (SECTORS - 1)
    table_ref[...] = jnp.where(label == sec_ref[...], 1.0, 0.0).astype(bf16)
    value = ret_ref[...]
    hi, lo = split2(value)
    hi_ref[:rows] = hi
    lo_ref[:rows] = lo
    hi_ref[rows:] = jnp.ones_like(hi_ref[rows:])
    lo_ref[rows:] = jnp.zeros_like(lo_ref[rows:])
    tail_ref[...] = ret_ref[rows - W :]
    acc = dot_nt(hi_ref[...], table_ref[...]) + dot_nt(lo_ref[...], table_ref[...])
    keep_ref[...] = acc[: rows + 8, :HALF]
    send_ref[...] = acc[: rows + 8, HALF:]


def sector_sums(core, returns, sector):
    rows, width = returns.shape
    half = jax.ShapeDtypeStruct((rows + 8, HALF), f32)
    return pl.pallas_call(
        sums_kernel,
        out_shape=(
            half,
            half,
            jax.ShapeDtypeStruct((SECTORS, width), bf16),
            jax.ShapeDtypeStruct((W, width), f32),
        ),
        in_specs=[
            pl.BlockSpec(memory_space=pltpu.SMEM),
            pl.BlockSpec(memory_space=pltpu.VMEM),
            pl.BlockSpec(memory_space=pltpu.VMEM),
        ],
        out_specs=[pl.BlockSpec(memory_space=pltpu.VMEM)] * 4,
        scratch_shapes=[pltpu.VMEM((rows + 16, width), bf16)] * 2,
        compiler_params=pltpu.CompilerParams(vmem_limit_bytes=24 * MIB),
        cost_estimate=pl.CostEstimate(
            flops=4 * rows * width * SECTORS, bytes_accessed=8 * rows * width, transcendentals=0
        ),
        name="sector_sums",
    )(core, returns, sector)


class Window:
    def __init__(self):
        self.rolled = {}
        self.sums = {8: [], 16: [], 32: []}

    def push(self, x, row):
        size = 1
        while size < 8:
            turned = pltpu.roll(x, size, 0)
            before = self.rolled.get(size, turned)
            self.rolled[size] = turned
            x = x + jnp.where(row < size, before, turned)
            size *= 2
        while size < W:
            seen = self.sums[size]
            seen.append(x)
            back = size // 8
            if len(seen) <= back:
                return None
            x = x + seen[-1 - back]
            size *= 2
        return x


def tile_at(index):
    return pl.ds(pl.multiple_of(index * LANES, LANES), LANES)


def rows_of(group):
    return slice(group * 8, group * 8 + 8)


def inverse_counts(first_step, inv_ref):
    position = lax.broadcasted_iota(jnp.int32, inv_ref.shape, 0) + (first_step + 1)
    inv_ref[...] = 1.0 / jnp.minimum(position, W).astype(f32)


def moments_body(load, inv, groups, mean_ref, crr_ref):
    row = lax.broadcasted_iota(jnp.int32, (8, LANES), 0)

    def tile(index, _):
        cols = tile_at(index)
        first, second = Window(), Window()
        for group in range(groups):
            ret = load(group, cols)
            total, squares = first.push(ret, row), second.push(ret * ret, row)
            if group >= W // 8:
                here = rows_of(group - W // 8)
                scale = inv(group - W // 8)
                mean = total * scale
                mean_ref[here, cols] = mean
                crr_ref[here, cols] = squares * scale - mean * mean
        return 0

    lax.fori_loop(0, mean_ref.shape[1] // LANES, tile, 0)


def moments_main_kernel(ret_ref, mean_ref, crr_ref):
    moments_body(
        lambda group, cols: ret_ref[rows_of(group), cols],
        lambda group: 1.0 / W,
        ret_ref.shape[0] // 8,
        mean_ref,
        crr_ref,
    )


def moments_head_kernel(info_ref, halo_ref, ret_ref, mean_ref, crr_ref, inv_ref):
    inverse_counts(info_ref[1], inv_ref)
    blocks = W // 8
    moments_body(
        lambda group, cols: halo_ref[rows_of(group), cols]
        if group < blocks
        else ret_ref[rows_of(group - blocks), cols],
        lambda group: inv_ref[rows_of(group)],
        2 * blocks,
        mean_ref,
        crr_ref,
    )


def sector_rows(means, inv, groups, starts, hi_ref, lo_ref, out):
    row = lax.broadcasted_iota(jnp.int32, (8, LANES), 0)
    first, second = Window(), Window()
    mean_parts, gain_parts = [], []
    for group in range(groups):
        mean = means[group]
        total, squares = first.push(mean, row), second.push(mean * mean, row)
        if group >= W // 8:
            scale = inv(group - W // 8)
            mean_f = total * scale
            mean_parts.append(mean_f)
            gain_parts.append(1.0 / (squares * scale - mean_f * mean_f + ridge_rate))
    for start, parts in zip(starts, (means, mean_parts, gain_parts)):
        if start is None:
            continue
        for pair in range(0, len(parts), 2):
            hi, lo = split2(jnp.concatenate(parts[pair : pair + 2], axis=0))
            here = slice(start + pair * 8, start + pair * 8 + 16)
            hi_ref[here, out] = hi
            lo_ref[here, out] = lo


def main_kernel(
    own_ref, other_ref, own_tail_ref, other_tail_ref, ret_ref, mean_ref, crr_ref, table_ref,
    var_ref, factor_ref, colsum_ref, hi_ref, lo_ref, spread_ref,
):
    rows = ret_ref.shape[0]
    main = rows - W
    blocks = W // 8
    for tile in range(SECTORS // LANES):
        here, tail = (own_ref, own_tail_ref) if tile < HALF // LANES else (other_ref, other_tail_ref)
        cols = pl.ds((tile * LANES) % HALF, LANES)
        scale = 1.0 / jnp.maximum(tail[W : W + 8, cols], 1.0)
        means = [
            (here[rows_of(g), cols] if g < main // 8 else tail[rows_of(g - main // 8), cols]) * scale
            for g in range(rows // 8)
        ]
        sector_rows(
            means, lambda g: 1.0 / W, rows // 8, (0, rows, rows + main), hi_ref, lo_ref,
            slice(tile * LANES, (tile + 1) * LANES),
        )
    row = lax.broadcasted_iota(jnp.int32, (8, LANES), 0)
    wide = spread_ref.shape[1]

    def chunk(index, _):
        outer = pl.ds(pl.multiple_of(index * wide, wide), wide)
        spread_ref[...] = dot_nn(hi_ref[...], table_ref[:, outer]) + dot_nn(
            lo_ref[...], table_ref[:, outer]
        )
        for tile in range(wide // LANES):
            inner = slice(tile * LANES, (tile + 1) * LANES)
            cols = pl.ds(pl.multiple_of(index * wide + tile * LANES, LANES), LANES)
            cross = Window()
            total = jnp.zeros((8, LANES), f32)
            for group in range(rows // 8):
                factor = spread_ref[rows_of(group), inner]
                if group < blocks:
                    factor_ref[rows_of(group), cols] = factor
                product = cross.push(ret_ref[rows_of(group), cols] * factor, row)
                if group >= blocks:
                    g = group - blocks
                    mean_f = spread_ref[rows_of(rows // 8 + g), inner]
                    gain = spread_ref[rows_of((rows + main) // 8 + g), inner]
                    crf = product * (1.0 / W) - mean_ref[rows_of(g), cols] * mean_f
                    variance = crr_ref[rows_of(g), cols] - crf * crf * gain
                    var_ref[rows_of(g), cols] = (1.0 - shrink_weight) * variance
                    total = total + variance
            colsum_ref[:, cols] = total
        return 0

    lax.fori_loop(0, ret_ref.shape[1] // wide, chunk, 0)


def head_kernel(
    info_ref, own_ref, other_ref, counts_own_ref, counts_other_ref, prior_own_ref, prior_other_ref,
    halo_ref, ret_ref, factor_ref, mean_ref, crr_ref, colsum_ref, table_ref,
    var_ref, totals_ref, hi_ref, lo_ref, spread_ref, inv_ref, parts_ref,
):
    blocks = W // 8
    inverse_counts(info_ref[1], inv_ref)
    for tile in range(SECTORS // LANES):
        mine = tile < HALF // LANES
        here, prior, counts = (
            (own_ref, prior_own_ref, counts_own_ref)
            if mine
            else (other_ref, prior_other_ref, counts_other_ref)
        )
        cols = pl.ds((tile * LANES) % HALF, LANES)
        scale = 1.0 / jnp.maximum(counts[W : W + 8, cols], 1.0)
        means = [
            (prior[rows_of(g), cols] if g < blocks else here[rows_of(g - blocks), cols]) * scale
            for g in range(2 * blocks)
        ]
        sector_rows(
            means, lambda g: inv_ref[rows_of(g)], 2 * blocks, (0, 2 * W, 3 * W), hi_ref, lo_ref,
            slice(tile * LANES, (tile + 1) * LANES),
        )
    row = lax.broadcasted_iota(jnp.int32, (8, LANES), 0)
    wide = spread_ref.shape[1]

    def chunk(index, _):
        outer = pl.ds(pl.multiple_of(index * wide, wide), wide)
        spread_ref[...] = dot_nn(hi_ref[...], table_ref[:, outer]) + dot_nn(
            lo_ref[...], table_ref[:, outer]
        )
        for tile in range(wide // LANES):
            inner = slice(tile * LANES, (tile + 1) * LANES)
            cols = pl.ds(pl.multiple_of(index * wide + tile * LANES, LANES), LANES)
            cross = Window()
            total = colsum_ref[:, cols]
            for group in range(2 * blocks):
                g = group - blocks
                if g < 0:
                    product = halo_ref[rows_of(group), cols] * spread_ref[rows_of(group), inner]
                else:
                    product = ret_ref[rows_of(g), cols] * factor_ref[rows_of(g), cols]
                product = cross.push(product, row)
                if g >= 0:
                    mean_f = spread_ref[rows_of(2 * blocks + g), inner]
                    gain = spread_ref[rows_of(3 * blocks + g), inner]
                    crf = product * inv_ref[rows_of(g)] - mean_ref[rows_of(g), cols] * mean_f
                    variance = crr_ref[rows_of(g), cols] - crf * crf * gain
                    var_ref[rows_of(g), cols] = (1.0 - shrink_weight) * variance
                    total = total + variance
            hi = total.astype(bf16).astype(f32)
            mid = (total - hi).astype(bf16).astype(f32)
            parts_ref[:, cols] = jnp.concatenate(
                [hi, mid, total - hi - mid, jnp.zeros_like(hi)], axis=0
            ).astype(bf16)
        return 0

    lax.fori_loop(0, ret_ref.shape[1] // wide, chunk, 0)
    total = jnp.sum(dot_nt(parts_ref[...], table_ref[...]), axis=0, keepdims=True)
    swapped = jnp.concatenate([total[:, HALF:], total[:, :HALF]], axis=1)
    total = jnp.where(info_ref[0] == 0, total, swapped)
    totals_ref[...] = jnp.broadcast_to(total, totals_ref.shape)


SMEM = pl.BlockSpec(memory_space=pltpu.SMEM)
VMEM = pl.BlockSpec(memory_space=pltpu.VMEM)


def kernel_call(body, outs, scalars, arrays, scratch=(), flops=0, moved=0):
    return kernel_of(body, outs, scalars, arrays, scratch, flops, moved)


def kernel_of(body, outs, scalars, arrays, scratch, flops, moved):
    return pl.pallas_call(
        body,
        out_shape=tuple(jax.ShapeDtypeStruct(shape, f32) for shape in outs),
        in_specs=[SMEM] * len(scalars) + [VMEM] * len(arrays),
        out_specs=[VMEM] * len(outs),
        scratch_shapes=list(scratch),
        compiler_params=pltpu.CompilerParams(vmem_limit_bytes=24 * MIB),
        cost_estimate=pl.CostEstimate(flops=flops, bytes_accessed=moved, transcendentals=0),
    )(*scalars, *arrays)


def shrink_kernel(
    all_steps, core_ref, parts_ref, cown_ref, cother_ref, table_ref, head_ref, main_ref, out_ref, pooled_ref
):
    step = pl.program_id(0)

    @pl.when(step == 0)
    def _():
        total = jnp.sum(parts_ref[...], axis=0, keepdims=True)
        swapped = jnp.concatenate([total[:, HALF:], total[:, :HALF]], axis=1)
        total = jnp.where(core_ref[0] == 0, total, swapped)
        count = jnp.concatenate([cown_ref[W : W + 1], cother_ref[W : W + 1]], axis=1)
        mean = total / (all_steps * jnp.maximum(count, 1.0))
        spread = dot_nn(split3_rows(shrink_weight * mean), table_ref[...])
        pooled_ref[...] = jnp.broadcast_to(
            jnp.sum(spread, axis=0, keepdims=True), pooled_ref.shape
        )
        out_ref[...] = head_ref[...] + pooled_ref[0:1]

    @pl.when(step > 0)
    def _():
        out_ref[...] = main_ref[...] + pooled_ref[0:1]


def shrink(all_steps, core, parts, own, other, table, head, main):
    width = head.shape[1]
    rows = head.shape[0] + main.shape[0]
    fixed = lambda a: pl.BlockSpec(a.shape, lambda i: (0, 0))
    return pl.pallas_call(
        functools.partial(shrink_kernel, float(all_steps)),
        grid=(rows // W,),
        out_shape=jax.ShapeDtypeStruct((rows, width), f32),
        in_specs=[
            SMEM,
            fixed(parts),
            fixed(own),
            fixed(other),
            fixed(table),
            fixed(head),
            pl.BlockSpec((W, width), lambda i: (jnp.maximum(i - 1, 0), 0)),
        ],
        out_specs=pl.BlockSpec((W, width), lambda i: (i, 0)),
        scratch_shapes=[pltpu.VMEM((8, width), f32)],
        compiler_params=pltpu.CompilerParams(vmem_limit_bytes=24 * MIB),
        cost_estimate=pl.CostEstimate(
            flops=2 * rows * width, bytes_accessed=8 * rows * width, transcendentals=0
        ),
        name="shrink",
    )(core, parts, own, other, table, head, main)


def swap(value, axis, bit):
    return lax.ppermute(value, axis, [(i, i ^ bit) for i in range(lax.axis_size(axis))])


def ahead(value, axis):
    return lax.ppermute(value, axis, [(i, i + 1) for i in range(lax.axis_size(axis) - 1)])


def across(value, axis):
    bit = 2
    while bit < lax.axis_size(axis):
        value = value + swap(value, axis, bit)
        bit *= 2
    return value


def step(returns, sector):
    rows, width = returns.shape
    main = rows - W
    n_time, n_series = lax.axis_size("tm"), lax.axis_size("series")
    core = (lax.axis_index("series") % 2).astype(jnp.int32)
    first_step = (lax.axis_index("tm") * rows).astype(jnp.int32)
    info = jnp.stack([core, first_step])
    keep, send, table, tail = sector_sums(info, returns, sector[None, :])
    halo = ahead(tail, "tm")
    swapped = swap(send, "series", 1)
    own_tail = across(keep[main:] + swapped[main:], "series")
    own = across(keep[:main] + swapped[:main], "series")
    prior_own = ahead(own_tail, "tm")
    other_tail = swap(own_tail, "series", 1)
    other = swap(own, "series", 1)
    prior_other = swap(prior_own, "series", 1)
    wide = 2 * LANES
    lhs = 3 * rows - 2 * W
    mean, crr = kernel_call(
        moments_main_kernel, [(main, width)] * 2, [], [returns],
        flops=40 * main * width, moved=12 * main * width,
    )
    mean_head, crr_head = kernel_call(
        moments_head_kernel, [(W, width)] * 2, [info], [halo, returns],
        scratch=[pltpu.VMEM((W, LANES), f32)], flops=40 * W * width, moved=12 * W * width,
    )
    var, factor, colsum = kernel_call(
        main_kernel, [(main, width), (W, width), (8, width)], [],
        [own, other, own_tail, other_tail, returns, mean, crr, table],
        scratch=[pltpu.VMEM((lhs, SECTORS), bf16)] * 2 + [pltpu.VMEM((lhs, wide), f32)],
        flops=4 * lhs * width * SECTORS, moved=12 * rows * width,
    )
    var_head, totals = kernel_call(
        head_kernel, [(W, width), (n_time * n_series, SECTORS)], [info],
        [own, other, own_tail, other_tail, prior_own, prior_other, halo, returns, factor,
         mean_head, crr_head, colsum, table],
        scratch=[pltpu.VMEM((4 * W, SECTORS), bf16)] * 2
        + [pltpu.VMEM((4 * W, wide), f32), pltpu.VMEM((W, LANES), f32), pltpu.VMEM((32, width), bf16)],
        flops=16 * W * width * SECTORS, moved=12 * W * width,
    )
    parts = lax.all_to_all(totals, ("tm", "series"), 0, 0)
    return shrink(n_time * rows, info, parts, own_tail, other_tail, table, var_head, var)


def solution(mesh):
    placed = (P("tm", "series"), P("series"))
    return jax.shard_map(
        step, mesh=mesh, in_specs=placed, out_specs=P("tm", "series"), check_vma=False
    )
```

```python
import functools

import jax
import jax.numpy as jnp
from jax import lax
from jax.experimental import pallas as pl
from jax.experimental.pallas import tpu as pltpu
from jax.sharding import PartitionSpec as P


W = 64
SECTORS = 512
HALF = SECTORS // 2
LANES = 128

ridge_rate = 0.05
shrink_weight = 0.3

f32 = jnp.float32
bf16 = jnp.bfloat16
MIB = 1024 * 1024


def dot_nn(a, b):
    return lax.dot_general(a, b, (((1,), (0,)), ((), ())), preferred_element_type=f32)


def dot_nt(a, b):
    return lax.dot_general(a, b, (((1,), (1,)), ((), ())), preferred_element_type=f32)


def split2(x):
    hi = x.astype(bf16)
    return hi, (x - hi.astype(f32)).astype(bf16)


def split3_rows(x):
    hi = x.astype(bf16).astype(f32)
    rest = x - hi
    mid = rest.astype(bf16).astype(f32)
    low = rest - mid
    row = lax.broadcasted_iota(jnp.int32, (16, x.shape[1]), 0)
    return jnp.where(row == 0, hi, jnp.where(row == 1, mid, jnp.where(row == 2, low, 0.0))).astype(bf16)


def sums_kernel(
    core_ref, ret_hbm, sec_hbm, keep_ref, send_ref, table_ref, tail_ref,
    sec_ref, ret_ref, left_ref, acc_ref, sec_sem, tail_sem, ret_sems,
):
    rows, _ = ret_hbm.shape
    chunks, wide = ret_ref.shape[0], ret_ref.shape[2]
    height = rows + 16
    sec_copy = pltpu.make_async_copy(sec_hbm, sec_ref, sec_sem)
    sec_copy.start()
    copies = []
    for c in range(chunks):
        copy = pltpu.make_async_copy(
            ret_hbm.at[:, pl.ds(c * wide, wide)], ret_ref.at[c], ret_sems.at[c]
        )
        copy.start()
        copies.append(copy)
    tail_copy = pltpu.make_async_copy(ret_hbm.at[pl.ds(rows - W, W)], tail_ref, tail_sem)
    tail_copy.start()
    core = core_ref[0]
    left_ref[rows:height] = jnp.ones((16, wide), bf16)
    left_ref[height + rows :] = jnp.zeros((16, wide), bf16)
    sec_copy.wait()
    for c in range(chunks):
        cols = slice(c * wide, (c + 1) * wide)
        label = lax.broadcasted_iota(jnp.int32, (SECTORS, wide), 0)
        label = (label + core * HALF) & (SECTORS - 1)
        table_ref[:, cols] = jnp.where(label == sec_ref[:, cols], 1.0, 0.0).astype(bf16)
    for c in range(chunks):
        copies[c].wait()
        hi, lo = split2(ret_ref[c])
        left_ref[:rows] = hi
        left_ref[height : height + rows] = lo
        part = dot_nt(left_ref[...], table_ref[:, c * wide : (c + 1) * wide])
        part = part[: rows + 8] + part[height : height + rows + 8]
        if c == 0:
            acc_ref[...] = part
        elif c < chunks - 1:
            acc_ref[...] += part
        else:
            part = acc_ref[...] + part
            keep_ref[...] = part[:, :HALF]
            send_ref[...] = part[:, HALF:]
    tail_copy.wait()


def sector_sums(core, returns, sector):
    rows, width = returns.shape
    chunks = 4
    wide = width // chunks
    half = jax.ShapeDtypeStruct((rows + 8, HALF), f32)
    hbm = pl.BlockSpec(memory_space=pltpu.HBM)
    return pl.pallas_call(
        sums_kernel,
        out_shape=(
            half,
            half,
            jax.ShapeDtypeStruct((SECTORS, width), bf16),
            jax.ShapeDtypeStruct((W, width), f32),
        ),
        in_specs=[pl.BlockSpec(memory_space=pltpu.SMEM), hbm, hbm],
        out_specs=[pl.BlockSpec(memory_space=pltpu.VMEM)] * 4,
        scratch_shapes=[
            pltpu.VMEM((1, width), jnp.int32),
            pltpu.VMEM((chunks, rows, wide), f32),
            pltpu.VMEM((2 * rows + 32, wide), bf16),
            pltpu.VMEM((rows + 8, SECTORS), f32),
            pltpu.SemaphoreType.DMA,
            pltpu.SemaphoreType.DMA,
            pltpu.SemaphoreType.DMA((chunks,)),
        ],
        compiler_params=pltpu.CompilerParams(vmem_limit_bytes=24 * MIB),
        cost_estimate=pl.CostEstimate(
            flops=4 * rows * width * SECTORS, bytes_accessed=8 * rows * width, transcendentals=0
        ),
        name="sector_sums",
    )(core, returns, sector)


class Window:
    def __init__(self):
        self.rolled = {}
        self.sums = {8: [], 16: [], 32: []}

    def push(self, x, row):
        size = 1
        while size < 8:
            turned = pltpu.roll(x, size, 0)
            before = self.rolled.get(size, turned)
            self.rolled[size] = turned
            x = x + jnp.where(row < size, before, turned)
            size *= 2
        while size < W:
            seen = self.sums[size]
            seen.append(x)
            back = size // 8
            if len(seen) <= back:
                return None
            x = x + seen[-1 - back]
            size *= 2
        return x


def tile_at(index):
    return pl.ds(pl.multiple_of(index * LANES, LANES), LANES)


def rows_of(group):
    return slice(group * 8, group * 8 + 8)


def inverse_counts(first_step, inv_ref):
    position = lax.broadcasted_iota(jnp.int32, inv_ref.shape, 0) + (first_step + 1)
    inv_ref[...] = 1.0 / jnp.minimum(position, W).astype(f32)


def moments_body(load, inv, groups, mean_ref, crr_ref):
    row = lax.broadcasted_iota(jnp.int32, (8, LANES), 0)

    def tile(index, _):
        cols = tile_at(index)
        first, second = Window(), Window()
        for group in range(groups):
            ret = load(group, cols)
            total, squares = first.push(ret, row), second.push(ret * ret, row)
            if group >= W // 8:
                here = rows_of(group - W // 8)
                scale = inv(group - W // 8)
                mean = total * scale
                mean_ref[here, cols] = mean
                crr_ref[here, cols] = squares * scale - mean * mean
        return 0

    lax.fori_loop(0, mean_ref.shape[1] // LANES, tile, 0)


def moments_main_kernel(ret_ref, mean_ref, crr_ref):
    moments_body(
        lambda group, cols: ret_ref[rows_of(group), cols],
        lambda group: 1.0 / W,
        ret_ref.shape[0] // 8,
        mean_ref,
        crr_ref,
    )


def moments_head_kernel(info_ref, halo_ref, ret_ref, mean_ref, crr_ref, inv_ref):
    inverse_counts(info_ref[1], inv_ref)
    blocks = W // 8
    moments_body(
        lambda group, cols: halo_ref[rows_of(group), cols]
        if group < blocks
        else ret_ref[rows_of(group - blocks), cols],
        lambda group: inv_ref[rows_of(group)],
        2 * blocks,
        mean_ref,
        crr_ref,
    )


def sector_rows(means, inv, groups, starts, hi_ref, lo_ref, out, kept=None):
    row = lax.broadcasted_iota(jnp.int32, (8, LANES), 0)
    first, second = Window(), Window()
    mean_parts, gain_parts = [], []
    for group in range(groups):
        mean = means[group]
        total, squares = first.push(mean, row), second.push(mean * mean, row)
        if group >= W // 8:
            scale = inv(group - W // 8)
            mean_f = total * scale
            mean_parts.append(mean_f)
            gain_parts.append(1.0 / (squares * scale - mean_f * mean_f + ridge_rate))
    for start, parts in zip(starts, (means[:kept], mean_parts, gain_parts)):
        for pair in range(0, len(parts), 2):
            hi, lo = split2(jnp.concatenate(parts[pair : pair + 2], axis=0))
            here = slice(start + pair * 8, start + pair * 8 + 16)
            hi_ref[here, out] = hi
            lo_ref[here, out] = lo


def pipelined(left_hi, left_lo, table_ref, buffers, work):
    even, odd = buffers
    wide = even.shape[1]
    chunks = table_ref.shape[1] // wide

    def fill(buffer, index):
        cols = pl.ds(pl.multiple_of(index * wide, wide), wide)
        buffer[...] = dot_nn(left_hi[...], table_ref[:, cols]) + dot_nn(
            left_lo[...], table_ref[:, cols]
        )

    fill(even, 0)

    def pair(j, _):
        fill(odd, 2 * j + 1)
        work(even, 2 * j)
        fill(even, 2 * j + 2)
        work(odd, 2 * j + 1)
        return 0

    lax.fori_loop(0, chunks // 2 - 1, pair, 0)
    fill(odd, chunks - 1)
    work(even, chunks - 2)
    work(odd, chunks - 1)


def main_kernel(
    own_ref, other_ref, own_tail_ref, other_tail_ref, ret_ref, mean_ref, crr_ref, table_ref,
    var_ref, factor_ref, colsum_ref, hi_ref, lo_ref, even_ref, odd_ref,
):
    rows = ret_ref.shape[0]
    main = rows - W
    blocks = W // 8
    for tile in range(SECTORS // LANES):
        here, tail = (own_ref, own_tail_ref) if tile < HALF // LANES else (other_ref, other_tail_ref)
        cols = pl.ds((tile * LANES) % HALF, LANES)
        scale = 1.0 / jnp.maximum(tail[W : W + 8, cols], 1.0)
        means = [
            (here[rows_of(g), cols] if g < main // 8 else tail[rows_of(g - main // 8), cols]) * scale
            for g in range(rows // 8)
        ]
        sector_rows(
            means, lambda g: 1.0 / W, rows // 8, (0, rows, rows + main), hi_ref, lo_ref,
            slice(tile * LANES, (tile + 1) * LANES),
        )
    row = lax.broadcasted_iota(jnp.int32, (8, LANES), 0)
    wide = even_ref.shape[1]

    def chunk(spread_ref, index):
        for tile in range(wide // LANES):
            inner = slice(tile * LANES, (tile + 1) * LANES)
            cols = pl.ds(pl.multiple_of(index * wide + tile * LANES, LANES), LANES)
            cross = Window()
            total = jnp.zeros((8, LANES), f32)
            for group in range(rows // 8):
                factor = spread_ref[rows_of(group), inner]
                if group < blocks:
                    factor_ref[rows_of(group), cols] = factor
                product = cross.push(ret_ref[rows_of(group), cols] * factor, row)
                if group >= blocks:
                    g = group - blocks
                    mean_f = spread_ref[rows_of(rows // 8 + g), inner]
                    gain = spread_ref[rows_of((rows + main) // 8 + g), inner]
                    crf = product * (1.0 / W) - mean_ref[rows_of(g), cols] * mean_f
                    variance = crr_ref[rows_of(g), cols] - crf * crf * gain
                    var_ref[rows_of(g), cols] = (1.0 - shrink_weight) * variance
                    total = total + variance
            colsum_ref[:, cols] = total

    pipelined(hi_ref, lo_ref, table_ref, (even_ref, odd_ref), chunk)


def head_kernel(
    info_ref, own_ref, other_ref, counts_own_ref, counts_other_ref, prior_own_ref, prior_other_ref,
    halo_ref, ret_ref, factor_ref, mean_ref, crr_ref, colsum_ref, table_ref,
    var_ref, totals_ref, hi_ref, lo_ref, even_ref, odd_ref, inv_ref, parts_ref,
):
    blocks = W // 8
    inverse_counts(info_ref[1], inv_ref)
    for tile in range(SECTORS // LANES):
        mine = tile < HALF // LANES
        here, prior, counts = (
            (own_ref, prior_own_ref, counts_own_ref)
            if mine
            else (other_ref, prior_other_ref, counts_other_ref)
        )
        cols = pl.ds((tile * LANES) % HALF, LANES)
        scale = 1.0 / jnp.maximum(counts[W : W + 8, cols], 1.0)
        means = [
            (prior[rows_of(g), cols] if g < blocks else here[rows_of(g - blocks), cols]) * scale
            for g in range(2 * blocks)
        ]
        sector_rows(
            means, lambda g: inv_ref[rows_of(g)], 2 * blocks, (0, W, 2 * W), hi_ref, lo_ref,
            slice(tile * LANES, (tile + 1) * LANES), blocks,
        )
    row = lax.broadcasted_iota(jnp.int32, (8, LANES), 0)
    wide = even_ref.shape[1]

    def chunk(spread_ref, index):
        for tile in range(wide // LANES):
            inner = slice(tile * LANES, (tile + 1) * LANES)
            cols = pl.ds(pl.multiple_of(index * wide + tile * LANES, LANES), LANES)
            cross = Window()
            total = colsum_ref[:, cols]
            for group in range(2 * blocks):
                g = group - blocks
                if g < 0:
                    product = halo_ref[rows_of(group), cols] * spread_ref[rows_of(group), inner]
                else:
                    product = ret_ref[rows_of(g), cols] * factor_ref[rows_of(g), cols]
                product = cross.push(product, row)
                if g >= 0:
                    mean_f = spread_ref[rows_of(blocks + g), inner]
                    gain = spread_ref[rows_of(2 * blocks + g), inner]
                    crf = product * inv_ref[rows_of(g)] - mean_ref[rows_of(g), cols] * mean_f
                    variance = crr_ref[rows_of(g), cols] - crf * crf * gain
                    var_ref[rows_of(g), cols] = (1.0 - shrink_weight) * variance
                    total = total + variance
            hi = total.astype(bf16).astype(f32)
            mid = (total - hi).astype(bf16).astype(f32)
            parts_ref[:, cols] = jnp.concatenate(
                [hi, mid, total - hi - mid, jnp.zeros_like(hi)], axis=0
            ).astype(bf16)

    pipelined(hi_ref, lo_ref, table_ref, (even_ref, odd_ref), chunk)
    total = jnp.sum(dot_nt(parts_ref[...], table_ref[...]), axis=0, keepdims=True)
    swapped = jnp.concatenate([total[:, HALF:], total[:, :HALF]], axis=1)
    total = jnp.where(info_ref[0] == 0, total, swapped)
    totals_ref[...] = jnp.broadcast_to(total, totals_ref.shape)


SMEM = pl.BlockSpec(memory_space=pltpu.SMEM)
VMEM = pl.BlockSpec(memory_space=pltpu.VMEM)


def kernel_call(body, outs, scalars, arrays, scratch=(), flops=0, moved=0):
    return kernel_of(body, outs, scalars, arrays, scratch, flops, moved)


def kernel_of(body, outs, scalars, arrays, scratch, flops, moved):
    return pl.pallas_call(
        body,
        out_shape=tuple(jax.ShapeDtypeStruct(shape, f32) for shape in outs),
        in_specs=[SMEM] * len(scalars) + [VMEM] * len(arrays),
        out_specs=[VMEM] * len(outs),
        scratch_shapes=list(scratch),
        compiler_params=pltpu.CompilerParams(vmem_limit_bytes=24 * MIB),
        cost_estimate=pl.CostEstimate(flops=flops, bytes_accessed=moved, transcendentals=0),
    )(*scalars, *arrays)


def shrink_kernel(
    all_steps, core_ref, parts_ref, cown_ref, cother_ref, table_ref, head_ref, main_ref, out_hbm, out_ref, sems
):
    total = jnp.sum(parts_ref[...], axis=0, keepdims=True)
    swapped = jnp.concatenate([total[:, HALF:], total[:, :HALF]], axis=1)
    total = jnp.where(core_ref[0] == 0, total, swapped)
    count = jnp.concatenate([cown_ref[W : W + 1], cother_ref[W : W + 1]], axis=1)
    mean = total / (all_steps * jnp.maximum(count, 1.0))
    left = split3_rows(shrink_weight * mean)
    chunks, _, wide = out_ref.shape
    copies = []
    for c in range(chunks):
        cols = slice(c * wide, (c + 1) * wide)
        pooled = jnp.sum(dot_nn(left, table_ref[:, cols]), axis=0, keepdims=True)
        out_ref[c, :W] = head_ref[:, cols] + pooled
        out_ref[c, W:] = main_ref[:, cols] + pooled
        copy = pltpu.make_async_copy(out_ref.at[c], out_hbm.at[:, pl.ds(c * wide, wide)], sems.at[c])
        copy.start()
        copies.append(copy)
    for copy in copies:
        copy.wait()


def shrink(all_steps, core, parts, own, other, table, head, main):
    width = head.shape[1]
    rows = head.shape[0] + main.shape[0]
    chunks = 4
    return pl.pallas_call(
        functools.partial(shrink_kernel, float(all_steps)),
        out_shape=jax.ShapeDtypeStruct((rows, width), f32),
        in_specs=[SMEM] + [VMEM] * 6,
        out_specs=pl.BlockSpec(memory_space=pltpu.HBM),
        scratch_shapes=[
            pltpu.VMEM((chunks, rows, width // chunks), f32),
            pltpu.SemaphoreType.DMA((chunks,)),
        ],
        compiler_params=pltpu.CompilerParams(vmem_limit_bytes=24 * MIB),
        cost_estimate=pl.CostEstimate(
            flops=2 * rows * width, bytes_accessed=8 * rows * width, transcendentals=0
        ),
        name="shrink",
    )(core, parts, own, other, table, head, main)


def swap(value, axis, bit):
    return lax.ppermute(value, axis, [(i, i ^ bit) for i in range(lax.axis_size(axis))])


def ahead(value, axis):
    return lax.ppermute(value, axis, [(i, i + 1) for i in range(lax.axis_size(axis) - 1)])


def across(value, axis):
    bit = 2
    while bit < lax.axis_size(axis):
        value = value + swap(value, axis, bit)
        bit *= 2
    return value


def step(returns, sector):
    rows, width = returns.shape
    main = rows - W
    n_time, n_series = lax.axis_size("tm"), lax.axis_size("series")
    core = (lax.axis_index("series") % 2).astype(jnp.int32)
    first_step = (lax.axis_index("tm") * rows).astype(jnp.int32)
    info = jnp.stack([core, first_step])
    keep, send, table, tail = sector_sums(info, returns, sector[None, :])
    halo = ahead(tail, "tm")
    swapped = swap(send, "series", 1)
    own_tail = across(keep[main:] + swapped[main:], "series")
    own = across(keep[:main] + swapped[:main], "series")
    prior_own = ahead(own_tail, "tm")
    other_tail = swap(own_tail, "series", 1)
    other = swap(own, "series", 1)
    prior_other = swap(prior_own, "series", 1)
    wide = 2 * LANES
    lhs = 3 * rows - 2 * W
    mean, crr = kernel_call(
        moments_main_kernel, [(main, width)] * 2, [], [returns],
        flops=40 * main * width, moved=12 * main * width,
    )
    mean_head, crr_head = kernel_call(
        moments_head_kernel, [(W, width)] * 2, [info], [halo, returns],
        scratch=[pltpu.VMEM((W, LANES), f32)], flops=40 * W * width, moved=12 * W * width,
    )
    var, factor, colsum = kernel_call(
        main_kernel, [(main, width), (W, width), (8, width)], [],
        [own, other, own_tail, other_tail, returns, mean, crr, table],
        scratch=[pltpu.VMEM((lhs, SECTORS), bf16)] * 2 + [pltpu.VMEM((lhs, wide), f32)] * 2,
        flops=4 * lhs * width * SECTORS, moved=12 * rows * width,
    )
    var_head, totals = kernel_call(
        head_kernel, [(W, width), (n_time * n_series, SECTORS)], [info],
        [own, other, own_tail, other_tail, prior_own, prior_other, halo, returns, factor,
         mean_head, crr_head, colsum, table],
        scratch=[pltpu.VMEM((3 * W, SECTORS), bf16)] * 2
        + [pltpu.VMEM((3 * W, wide), f32)] * 2
        + [pltpu.VMEM((W, LANES), f32), pltpu.VMEM((32, width), bf16)],
        flops=16 * W * width * SECTORS, moved=12 * W * width,
    )
    parts = lax.all_to_all(totals, ("tm", "series"), 0, 0)
    return shrink(n_time * rows, info, parts, own_tail, other_tail, table, var_head, var)


def solution(mesh):
    placed = (P("tm", "series"), P("series"))
    return jax.shard_map(
        step, mesh=mesh, in_specs=placed, out_specs=P("tm", "series"), check_vma=False
    )
```

```python
import functools

import jax
import jax.numpy as jnp
from jax import lax
from jax.experimental import pallas as pl
from jax.experimental.pallas import tpu as pltpu
from jax.sharding import PartitionSpec as P


W = 64
SECTORS = 512
HALF = SECTORS // 2
LANES = 128

ridge_rate = 0.05
shrink_weight = 0.3

f32 = jnp.float32
bf16 = jnp.bfloat16
MIB = 1024 * 1024


def dot_nn(a, b):
    return lax.dot_general(a, b, (((1,), (0,)), ((), ())), preferred_element_type=f32)


def dot_nt(a, b):
    return lax.dot_general(a, b, (((1,), (1,)), ((), ())), preferred_element_type=f32)


def split2(x):
    hi = x.astype(bf16)
    return hi, (x - hi.astype(f32)).astype(bf16)


def split3_rows(x):
    hi = x.astype(bf16).astype(f32)
    rest = x - hi
    mid = rest.astype(bf16).astype(f32)
    low = rest - mid
    row = lax.broadcasted_iota(jnp.int32, (16, x.shape[1]), 0)
    return jnp.where(row == 0, hi, jnp.where(row == 1, mid, jnp.where(row == 2, low, 0.0))).astype(bf16)


def table_kernel(ret_hbm, sec_ref, core_ref, first_ref, table_ref, ret_ref, flip_ref, inv_ref, sem):
    copy = pltpu.make_async_copy(ret_hbm, ret_ref, sem)
    copy.start()
    wide = 4 * LANES
    flip_ref[...] = jnp.concatenate([core_ref[...]] * (SECTORS // LANES), axis=1)
    position = lax.broadcasted_iota(jnp.int32, inv_ref.shape, 0) + (first_ref[0:1] + 1)
    inv_ref[...] = 1.0 / jnp.minimum(position, W).astype(f32)
    for c in range(table_ref.shape[1] // wide):
        cols = slice(c * wide, (c + 1) * wide)
        label = lax.broadcasted_iota(jnp.int32, (SECTORS, wide), 0)
        table_ref[:, cols] = jnp.where(label == sec_ref[:, cols], 1.0, 0.0).astype(bf16)
    copy.wait()


def sums_kernel(ret_ref, table_ref, keep_ref, send_ref, tail_ref, left_ref):
    rows, width = ret_ref.shape
    height = rows + 16
    hi, lo = split2(ret_ref[...])
    left_ref[:rows] = hi
    left_ref[rows:height] = jnp.ones((16, width), bf16)
    left_ref[height : height + rows] = lo
    left_ref[height + rows :] = jnp.zeros((16, width), bf16)
    tail_ref[...] = ret_ref[rows - W :]
    part = dot_nt(left_ref[...], table_ref[...])
    part = part[: rows + 8] + part[height : height + rows + 8]
    keep_ref[...] = part[:, :HALF]
    send_ref[...] = part[:, HALF:]


class Window:
    def __init__(self):
        self.rolled = {}
        self.sums = {8: [], 16: [], 32: []}

    def push(self, x, row):
        size = 1
        while size < 8:
            turned = pltpu.roll(x, size, 0)
            before = self.rolled.get(size, turned)
            self.rolled[size] = turned
            x = x + jnp.where(row < size, before, turned)
            size *= 2
        while size < W:
            seen = self.sums[size]
            seen.append(x)
            back = size // 8
            if len(seen) <= back:
                return None
            x = x + seen[-1 - back]
            size *= 2
        return x


def tile_at(index):
    return pl.ds(pl.multiple_of(index * LANES, LANES), LANES)


def rows_of(group):
    return slice(group * 8, group * 8 + 8)


def moments_body(load, inv, groups, mean_ref, crr_ref):
    row = lax.broadcasted_iota(jnp.int32, (8, LANES), 0)

    def tile(index, _):
        cols = tile_at(index)
        first, second = Window(), Window()
        for group in range(groups):
            ret = load(group, cols)
            total, squares = first.push(ret, row), second.push(ret * ret, row)
            if group >= W // 8:
                here = rows_of(group - W // 8)
                scale = inv(group - W // 8)
                mean = total * scale
                mean_ref[here, cols] = mean
                crr_ref[here, cols] = squares * scale - mean * mean
        return 0

    lax.fori_loop(0, mean_ref.shape[1] // LANES, tile, 0)


def moments_main_kernel(ret_ref, mean_ref, crr_ref):
    moments_body(
        lambda group, cols: ret_ref[rows_of(group), cols],
        lambda group: 1.0 / W,
        ret_ref.shape[0] // 8,
        mean_ref,
        crr_ref,
    )


def moments_head_kernel(inv_ref, halo_ref, ret_ref, mean_ref, crr_ref):
    blocks = W // 8
    moments_body(
        lambda group, cols: halo_ref[rows_of(group), cols]
        if group < blocks
        else ret_ref[rows_of(group - blocks), cols],
        lambda group: inv_ref[rows_of(group)],
        2 * blocks,
        mean_ref,
        crr_ref,
    )


def sector_rows(means, inv, groups, starts, hi_ref, lo_ref, out, kept=None):
    row = lax.broadcasted_iota(jnp.int32, (8, LANES), 0)
    first, second = Window(), Window()
    mean_parts, gain_parts = [], []
    for group in range(groups):
        mean = means[group]
        total, squares = first.push(mean, row), second.push(mean * mean, row)
        if group >= W // 8:
            scale = inv(group - W // 8)
            mean_f = total * scale
            mean_parts.append(mean_f)
            gain_parts.append(1.0 / (squares * scale - mean_f * mean_f + ridge_rate))
    for start, parts in zip(starts, (means[:kept], mean_parts, gain_parts)):
        for pair in range(0, len(parts), 2):
            hi, lo = split2(jnp.concatenate(parts[pair : pair + 2], axis=0))
            here = slice(start + pair * 8, start + pair * 8 + 16)
            hi_ref[here, out] = hi
            lo_ref[here, out] = lo


def pipelined(fill, work, buffers, chunks):
    even, odd = buffers
    fill(even, 0)

    def pair(j, _):
        fill(odd, 2 * j + 1)
        work(even, 2 * j)
        fill(even, 2 * j + 2)
        work(odd, 2 * j + 1)
        return 0

    lax.fori_loop(0, chunks // 2 - 1, pair, 0)
    fill(odd, chunks - 1)
    work(even, chunks - 2)
    work(odd, chunks - 1)


def chunk_at(index, wide):
    return pl.ds(pl.multiple_of(index * wide, wide), wide)


def main_rows(sums_ref, tail_ref, hi_ref, lo_ref):
    main = sums_ref.shape[0]
    rows = main + W
    for tile in range(HALF // LANES):
        cols = slice(tile * LANES, (tile + 1) * LANES)
        scale = 1.0 / jnp.maximum(tail_ref[W : W + 8, cols], 1.0)
        means = [
            (sums_ref[rows_of(g), cols] if g < main // 8 else tail_ref[rows_of(g - main // 8), cols])
            * scale
            for g in range(rows // 8)
        ]
        sector_rows(
            means, lambda g: 1.0 / W, rows // 8, (0, rows, rows + main), hi_ref, lo_ref, cols
        )


def own_kernel(own_ref, own_tail_ref, table_ref, spread_ref, hi_ref, lo_ref):
    main_rows(own_ref, own_tail_ref, hi_ref, lo_ref)
    wide = 2 * LANES

    def chunk(index, _):
        cols = chunk_at(index, wide)
        table = table_ref[:HALF, cols]
        spread_ref[:, cols] = dot_nn(hi_ref[...], table) + dot_nn(lo_ref[...], table)
        return 0

    lax.fori_loop(0, table_ref.shape[1] // wide, chunk, 0)


def main_kernel(
    other_ref, other_tail_ref, spread_ref, ret_ref, mean_ref, crr_ref, table_ref,
    var_ref, factor_ref, colsum_ref, hi_ref, lo_ref, even_ref, odd_ref,
):
    rows = ret_ref.shape[0]
    main = rows - W
    blocks = W // 8
    main_rows(other_ref, other_tail_ref, hi_ref, lo_ref)
    row = lax.broadcasted_iota(jnp.int32, (8, LANES), 0)
    wide = even_ref.shape[1]

    def fill(buffer, index):
        cols = chunk_at(index, wide)
        table = table_ref[HALF:, cols]
        buffer[...] = spread_ref[:, cols] + dot_nn(hi_ref[...], table) + dot_nn(lo_ref[...], table)

    def work(spread_ref, index):
        for tile in range(wide // LANES):
            inner = slice(tile * LANES, (tile + 1) * LANES)
            cols = pl.ds(pl.multiple_of(index * wide + tile * LANES, LANES), LANES)
            cross = Window()
            total = jnp.zeros((8, LANES), f32)
            for group in range(rows // 8):
                factor = spread_ref[rows_of(group), inner]
                if group < blocks:
                    factor_ref[rows_of(group), cols] = factor
                product = cross.push(ret_ref[rows_of(group), cols] * factor, row)
                if group >= blocks:
                    g = group - blocks
                    mean_f = spread_ref[rows_of(rows // 8 + g), inner]
                    gain = spread_ref[rows_of((rows + main) // 8 + g), inner]
                    crf = product * (1.0 / W) - mean_ref[rows_of(g), cols] * mean_f
                    variance = crr_ref[rows_of(g), cols] - crf * crf * gain
                    var_ref[rows_of(g), cols] = (1.0 - shrink_weight) * variance
                    total = total + variance
            colsum_ref[:, cols] = total

    pipelined(fill, work, (even_ref, odd_ref), ret_ref.shape[1] // wide)


def head_kernel(
    inv_ref, flip_ref, own_ref, other_ref, counts_own_ref, counts_other_ref, prior_own_ref, prior_other_ref,
    halo_ref, ret_ref, factor_ref, mean_ref, crr_ref, colsum_ref, table_ref,
    var_ref, totals_ref, hi_ref, lo_ref, even_ref, odd_ref, acc_ref,
):
    blocks = W // 8
    acc_ref[...] = jnp.zeros_like(acc_ref)
    for tile in range(SECTORS // LANES):
        mine = tile < HALF // LANES
        here, prior, counts = (
            (own_ref, prior_own_ref, counts_own_ref)
            if mine
            else (other_ref, prior_other_ref, counts_other_ref)
        )
        cols = pl.ds((tile * LANES) % HALF, LANES)
        scale = 1.0 / jnp.maximum(counts[W : W + 8, cols], 1.0)
        means = [
            (prior[rows_of(g), cols] if g < blocks else here[rows_of(g - blocks), cols]) * scale
            for g in range(2 * blocks)
        ]
        sector_rows(
            means, lambda g: inv_ref[rows_of(g)], 2 * blocks, (0, W, 2 * W), hi_ref, lo_ref,
            slice(tile * LANES, (tile + 1) * LANES), blocks,
        )
    row = lax.broadcasted_iota(jnp.int32, (8, LANES), 0)
    wide = even_ref.shape[1]

    def fill(buffer, index):
        cols = chunk_at(index, wide)
        table = table_ref[:, cols]
        buffer[...] = dot_nn(hi_ref[...], table) + dot_nn(lo_ref[...], table)

    def work(spread_ref, index):
        parts = []
        for tile in range(wide // LANES):
            inner = slice(tile * LANES, (tile + 1) * LANES)
            cols = pl.ds(pl.multiple_of(index * wide + tile * LANES, LANES), LANES)
            cross = Window()
            total = colsum_ref[:, cols]
            for group in range(2 * blocks):
                g = group - blocks
                if g < 0:
                    product = halo_ref[rows_of(group), cols] * spread_ref[rows_of(group), inner]
                else:
                    product = ret_ref[rows_of(g), cols] * factor_ref[rows_of(g), cols]
                product = cross.push(product, row)
                if g >= 0:
                    mean_f = spread_ref[rows_of(blocks + g), inner]
                    gain = spread_ref[rows_of(2 * blocks + g), inner]
                    crf = product * inv_ref[rows_of(g)] - mean_ref[rows_of(g), cols] * mean_f
                    variance = crr_ref[rows_of(g), cols] - crf * crf * gain
                    var_ref[rows_of(g), cols] = (1.0 - shrink_weight) * variance
                    total = total + variance
            hi = total.astype(bf16).astype(f32)
            mid = (total - hi).astype(bf16).astype(f32)
            parts.append(
                jnp.concatenate([hi, mid, total - hi - mid, jnp.zeros_like(hi)], axis=0).astype(bf16)
            )
        acc_ref[...] += dot_nt(
            jnp.concatenate(parts, axis=1), table_ref[:, chunk_at(index, wide)]
        )

    pipelined(fill, work, (even_ref, odd_ref), ret_ref.shape[1] // wide)
    total = jnp.sum(acc_ref[...], axis=0, keepdims=True)
    swapped = jnp.concatenate([total[:, HALF:], total[:, :HALF]], axis=1)
    total = jnp.where(flip_ref[0:1] == 0, total, swapped)
    totals_ref[...] = jnp.broadcast_to(total, totals_ref.shape)


VMEM = pl.BlockSpec(memory_space=pltpu.VMEM)


def kernel_call(body, outs, arrays, scratch=(), flops=0, moved=0):
    return kernel_of(body, outs, arrays, scratch, flops, moved)


def kernel_of(body, outs, arrays, scratch, flops, moved):
    return pl.pallas_call(
        body,
        out_shape=tuple(o if hasattr(o, "dtype") else jax.ShapeDtypeStruct(o, f32) for o in outs),
        in_specs=[VMEM] * len(arrays),
        out_specs=[VMEM] * len(outs),
        scratch_shapes=list(scratch),
        compiler_params=pltpu.CompilerParams(vmem_limit_bytes=10 * MIB),
        cost_estimate=pl.CostEstimate(flops=flops, bytes_accessed=moved, transcendentals=0),
    )(*arrays)


def shrink_kernel(
    all_steps, flip_ref, parts_ref, cown_ref, cother_ref, table_ref, head_ref, main_ref, out_hbm, out_ref, sems
):
    total = jnp.sum(parts_ref[...], axis=0, keepdims=True)
    swapped = jnp.concatenate([total[:, HALF:], total[:, :HALF]], axis=1)
    total = jnp.where(flip_ref[0:1] == 0, total, swapped)
    count = jnp.concatenate([cown_ref[W : W + 1], cother_ref[W : W + 1]], axis=1)
    mean = total / (all_steps * jnp.maximum(count, 1.0))
    left = split3_rows(shrink_weight * mean)
    chunks, _, wide = out_ref.shape
    copies = []
    for c in range(chunks):
        cols = slice(c * wide, (c + 1) * wide)
        pooled = jnp.sum(dot_nn(left, table_ref[:, cols]), axis=0, keepdims=True)
        out_ref[c, :W] = head_ref[:, cols] + pooled
        out_ref[c, W:] = main_ref[:, cols] + pooled
        copy = pltpu.make_async_copy(out_ref.at[c], out_hbm.at[:, pl.ds(c * wide, wide)], sems.at[c])
        copy.start()
        copies.append(copy)
    for copy in copies:
        copy.wait()


def shrink(all_steps, flip, parts, own, other, table, head, main):
    width = head.shape[1]
    rows = head.shape[0] + main.shape[0]
    chunks = 4
    return pl.pallas_call(
        functools.partial(shrink_kernel, float(all_steps)),
        out_shape=jax.ShapeDtypeStruct((rows, width), f32),
        in_specs=[VMEM] * 7,
        out_specs=pl.BlockSpec(memory_space=pltpu.HBM),
        scratch_shapes=[
            pltpu.VMEM((chunks, rows, width // chunks), f32),
            pltpu.SemaphoreType.DMA((chunks,)),
        ],
        compiler_params=pltpu.CompilerParams(vmem_limit_bytes=10 * MIB),
        cost_estimate=pl.CostEstimate(
            flops=2 * rows * width, bytes_accessed=8 * rows * width, transcendentals=0
        ),
        name="shrink",
    )(flip, parts, own, other, table, head, main)


def swap(value, axis, bit):
    return lax.ppermute(value, axis, [(i, i ^ bit) for i in range(lax.axis_size(axis))])


def ahead(value, axis):
    return lax.ppermute(value, axis, [(i, i + 1) for i in range(lax.axis_size(axis) - 1)])


def across(value, axis):
    bit = 2
    while bit < lax.axis_size(axis):
        value = value + swap(value, axis, bit)
        bit *= 2
    return value


def step(returns, sector):
    rows, width = returns.shape
    main = rows - W
    n_time, n_series = lax.axis_size("tm"), lax.axis_size("series")
    core = (lax.axis_index("series") % 2).astype(jnp.int32)
    first_step = (lax.axis_index("tm") * rows).astype(jnp.int32)
    table, returns, flip, inv = pl.pallas_call(
        table_kernel,
        out_shape=(
            jax.ShapeDtypeStruct((SECTORS, width), bf16),
            jax.ShapeDtypeStruct((rows, width), f32),
            jax.ShapeDtypeStruct((8, SECTORS), jnp.int32),
            jax.ShapeDtypeStruct((W, LANES), f32),
        ),
        in_specs=[pl.BlockSpec(memory_space=pltpu.HBM)] + [VMEM] * 3,
        out_specs=[VMEM] * 4,
        scratch_shapes=[pltpu.SemaphoreType.DMA],
        compiler_params=pltpu.CompilerParams(vmem_limit_bytes=48 * MIB),
        name="table",
    )(
        returns,
        (sector ^ (core * HALF))[None, :],
        jnp.broadcast_to(core, (8, LANES)),
        jnp.broadcast_to(first_step, (8, LANES)),
    )
    keep, send, tail = kernel_call(
        sums_kernel, [(rows + 8, HALF), (rows + 8, HALF), (W, width)], [returns, table],
        scratch=[pltpu.VMEM((2 * rows + 32, width), bf16)],
        flops=4 * rows * width * SECTORS, moved=8 * rows * width,
    )
    halo = ahead(tail, "tm")
    swapped = swap(send, "series", 1)
    own_tail = across(keep[main:] + swapped[main:], "series")
    own = across(keep[:main] + swapped[:main], "series")
    prior_own = ahead(own_tail, "tm")
    other_tail = swap(own_tail, "series", 1)
    other = swap(own, "series", 1)
    prior_other = swap(prior_own, "series", 1)
    wide = 2 * LANES
    lhs = 3 * rows - 2 * W
    mean, crr = kernel_call(
        moments_main_kernel, [(main, width)] * 2, [returns],
        flops=40 * main * width, moved=12 * main * width,
    )
    mean_head, crr_head = kernel_call(
        moments_head_kernel, [(W, width)] * 2, [inv, halo, returns],
        flops=40 * W * width, moved=12 * W * width,
    )
    left = [pltpu.VMEM((lhs, HALF), bf16)] * 2
    (spread,) = kernel_call(
        own_kernel, [(lhs, width)], [own, own_tail, table], scratch=left,
        flops=2 * lhs * width * SECTORS, moved=4 * lhs * width,
    )
    var, factor, colsum = kernel_call(
        main_kernel, [(main, width), (W, width), (8, width)],
        [other, other_tail, spread, returns, mean, crr, table],
        scratch=left + [pltpu.VMEM((lhs, wide), f32)] * 2,
        flops=4 * lhs * width * SECTORS, moved=12 * rows * width,
    )
    var_head, totals = kernel_call(
        head_kernel, [(W, width), (n_time * n_series, SECTORS)],
        [inv, flip, own, other, own_tail, other_tail, prior_own, prior_other, halo, returns, factor,
         mean_head, crr_head, colsum, table],
        scratch=[pltpu.VMEM((3 * W, SECTORS), bf16)] * 2
        + [pltpu.VMEM((3 * W, wide), f32)] * 2
        + [pltpu.VMEM((32, SECTORS), f32)],
        flops=16 * W * width * SECTORS, moved=12 * W * width,
    )
    parts = lax.all_to_all(totals, ("tm", "series"), 0, 0)
    return shrink(n_time * rows, flip, parts, own_tail, other_tail, table, var_head, var)


def solution(mesh):
    placed = (P("tm", "series"), P("series"))
    return jax.shard_map(step, mesh=mesh, in_specs=placed, out_specs=P("tm", "series"), check_vma=False)
```

```python
import functools

import jax
import jax.numpy as jnp
from jax import lax
from jax.experimental import pallas as pl
from jax.experimental.pallas import tpu as pltpu
from jax.sharding import PartitionSpec as P


W = 64
SECTORS = 512
HALF = SECTORS // 2
LANES = 128

ridge_rate = 0.05
shrink_weight = 0.3

f32 = jnp.float32
bf16 = jnp.bfloat16
MIB = 1024 * 1024


def dot_nn(a, b):
    return lax.dot_general(a, b, (((1,), (0,)), ((), ())), preferred_element_type=f32)


def dot_nt(a, b):
    return lax.dot_general(a, b, (((1,), (1,)), ((), ())), preferred_element_type=f32)


def split2(x):
    hi = x.astype(bf16)
    return hi, (x - hi.astype(f32)).astype(bf16)


def split3_rows(x):
    hi = x.astype(bf16).astype(f32)
    rest = x - hi
    mid = rest.astype(bf16).astype(f32)
    low = rest - mid
    row = lax.broadcasted_iota(jnp.int32, (16, x.shape[1]), 0)
    return jnp.where(row == 0, hi, jnp.where(row == 1, mid, jnp.where(row == 2, low, 0.0))).astype(bf16)


def load_kernel(
    ret_hbm, sec_hbm, core_ref, first_ref,
    keep_ref, send_ref, table_ref, ret_ref, tail_ref, flip_ref, inv_ref,
    sec_ref, left_ref, acc_ref, sec_sem, tail_sem, ret_sems,
):
    rows, width = ret_ref.shape
    wide = left_ref.shape[1]
    height = rows + 16
    chunks = width // wide
    sec_copy = pltpu.make_async_copy(sec_hbm, sec_ref, sec_sem)
    sec_copy.start()
    copies = []
    for c in range(chunks):
        cols = pl.ds(c * wide, wide)
        copy = pltpu.make_async_copy(ret_hbm.at[:, cols], ret_ref.at[:, cols], ret_sems.at[c])
        copy.start()
        copies.append(copy)
    tail_copy = pltpu.make_async_copy(ret_hbm.at[pl.ds(rows - W, W)], tail_ref, tail_sem)
    tail_copy.start()
    flip_ref[...] = jnp.concatenate([core_ref[...]] * (SECTORS // LANES), axis=1)
    position = lax.broadcasted_iota(jnp.int32, inv_ref.shape, 0) + (first_ref[0:1] + 1)
    inv_ref[...] = 1.0 / jnp.minimum(position, W).astype(f32)
    left_ref[rows:height] = jnp.ones((16, wide), bf16)
    left_ref[height + rows :] = jnp.zeros((16, wide), bf16)
    turn = jnp.concatenate([core_ref[0:1] * HALF] * (wide // LANES), axis=1)
    sec_copy.wait()
    for c in range(chunks):
        cols = slice(c * wide, (c + 1) * wide)
        label = lax.broadcasted_iota(jnp.int32, (SECTORS, wide), 0)
        table_ref[:, cols] = jnp.where(label == (sec_ref[:, cols] ^ turn), 1.0, 0.0).astype(bf16)
    for c in range(chunks):
        cols = slice(c * wide, (c + 1) * wide)
        copies[c].wait()
        hi, lo = split2(ret_ref[:, cols])
        left_ref[:rows] = hi
        left_ref[height : height + rows] = lo
        part = dot_nt(left_ref[...], table_ref[:, cols])
        part = part[: rows + 8] + part[height : height + rows + 8]
        if c > 0:
            part = acc_ref[...] + part
        if c < chunks - 1:
            acc_ref[...] = part
    keep_ref[...] = part[:, :HALF]
    send_ref[...] = part[:, HALF:]
    tail_copy.wait()


class Window:
    def __init__(self):
        self.rolled = {}
        self.sums = {8: [], 16: [], 32: []}

    def push(self, x, row):
        size = 1
        while size < 8:
            turned = pltpu.roll(x, size, 0)
            before = self.rolled.get(size, turned)
            self.rolled[size] = turned
            x = x + jnp.where(row < size, before, turned)
            size *= 2
        while size < W:
            seen = self.sums[size]
            seen.append(x)
            back = size // 8
            if len(seen) <= back:
                return None
            x = x + seen[-1 - back]
            size *= 2
        return x


def tile_at(index):
    return pl.ds(pl.multiple_of(index * LANES, LANES), LANES)


def rows_of(group):
    return slice(group * 8, group * 8 + 8)


def moments_body(load, inv, groups, total_ref, crr_ref):
    row = lax.broadcasted_iota(jnp.int32, (8, LANES), 0)

    def tile(index, _):
        cols = tile_at(index)
        first, second = Window(), Window()
        for group in range(groups):
            ret = load(group, cols)
            total, squares = first.push(ret, row), second.push(ret * ret, row)
            if group >= W // 8:
                here = rows_of(group - W // 8)
                scale = inv(group - W // 8)
                mean = total * scale
                total_ref[here, cols] = total
                crr_ref[here, cols] = (1.0 - shrink_weight) * (squares * scale - mean * mean)
        return 0

    lax.fori_loop(0, total_ref.shape[1] // LANES, tile, 0)


def moments_main_kernel(ret_ref, mean_ref, crr_ref):
    moments_body(
        lambda group, cols: ret_ref[rows_of(group), cols],
        lambda group: 1.0 / W,
        ret_ref.shape[0] // 8,
        mean_ref,
        crr_ref,
    )


def moments_head_kernel(inv_ref, halo_ref, ret_ref, mean_ref, crr_ref):
    blocks = W // 8
    moments_body(
        lambda group, cols: halo_ref[rows_of(group), cols]
        if group < blocks
        else ret_ref[rows_of(group - blocks), cols],
        lambda group: inv_ref[rows_of(group)],
        2 * blocks,
        mean_ref,
        crr_ref,
    )


def sector_rows(means, inv, groups, starts, left_ref, out, low, kept=None):
    row = lax.broadcasted_iota(jnp.int32, (8, LANES), 0)
    first, second = Window(), Window()
    mean_parts, gain_parts = [], []
    for group in range(groups):
        mean = means[group]
        total, squares = first.push(mean, row), second.push(mean * mean, row)
        if group >= W // 8:
            scale = inv(group - W // 8)
            mean_f = total * scale
            spread = squares * scale - mean_f * mean_f + ridge_rate
            mean_parts.append(mean_f)
            gain_parts.append((1.0 - shrink_weight) * scale * scale / spread)
    for start, parts in zip(starts, (means[:kept], mean_parts, gain_parts)):
        for pair in range(0, len(parts), 2):
            hi, lo = split2(jnp.concatenate(parts[pair : pair + 2], axis=0))
            here = slice(start + pair * 8, start + pair * 8 + 16)
            left_ref[here, out : out + LANES] = hi
            left_ref[here, out + low : out + low + LANES] = lo


def pipelined(fill, work, buffers, chunks):
    even, odd = buffers
    fill(even, 0)

    def pair(j, _):
        fill(odd, 2 * j + 1)
        work(even, 2 * j)
        fill(even, 2 * j + 2)
        work(odd, 2 * j + 1)
        return 0

    lax.fori_loop(0, chunks // 2 - 1, pair, 0)
    fill(odd, chunks - 1)
    work(even, chunks - 2)
    work(odd, chunks - 1)


def chunk_at(index, wide):
    return pl.ds(pl.multiple_of(index * wide, wide), wide)


def main_rows(sums_ref, tail_ref, left_ref):
    main = sums_ref.shape[0]
    rows = main + W
    for tile in range(HALF // LANES):
        cols = slice(tile * LANES, (tile + 1) * LANES)
        scale = 1.0 / jnp.maximum(tail_ref[W : W + 8, cols], 1.0)
        means = [
            (sums_ref[rows_of(g), cols] if g < main // 8 else tail_ref[rows_of(g - main // 8), cols])
            * scale
            for g in range(rows // 8)
        ]
        sector_rows(
            means, lambda g: 1.0 / W, rows // 8, (0, rows, rows + main), left_ref, tile * LANES, HALF
        )


def twice(table):
    return jnp.concatenate([table, table], axis=0)


def own_kernel(own_ref, own_tail_ref, table_ref, spread_ref, left_ref):
    main_rows(own_ref, own_tail_ref, left_ref)
    wide = 4 * LANES
    for index in range(table_ref.shape[1] // wide):
        cols = slice(index * wide, (index + 1) * wide)
        spread_ref[:, cols] = dot_nn(left_ref[...], twice(table_ref[:HALF, cols]))


def main_kernel(
    other_ref, other_tail_ref, spread_ref, ret_ref, total_ref, crr_ref, table_ref,
    var_ref, factor_ref, colsum_ref, left_ref, even_ref, odd_ref,
):
    rows = ret_ref.shape[0]
    main = rows - W
    blocks = W // 8
    main_rows(other_ref, other_tail_ref, left_ref)
    row = lax.broadcasted_iota(jnp.int32, (8, LANES), 0)
    wide = even_ref.shape[1]

    def fill(buffer, index):
        cols = chunk_at(index, wide)
        buffer[...] = spread_ref[:, cols] + dot_nn(left_ref[...], twice(table_ref[HALF:, cols]))

    def work(spread_ref, index):
        for tile in range(wide // LANES):
            inner = slice(tile * LANES, (tile + 1) * LANES)
            cols = pl.ds(pl.multiple_of(index * wide + tile * LANES, LANES), LANES)
            cross = Window()
            total = jnp.zeros((8, LANES), f32)
            for group in range(rows // 8):
                factor = spread_ref[rows_of(group), inner]
                if group < blocks:
                    factor_ref[rows_of(group), cols] = factor
                product = cross.push(ret_ref[rows_of(group), cols] * factor, row)
                if group >= blocks:
                    g = group - blocks
                    mean_f = spread_ref[rows_of(rows // 8 + g), inner]
                    gain = spread_ref[rows_of((rows + main) // 8 + g), inner]
                    crf = product - total_ref[rows_of(g), cols] * mean_f
                    variance = crr_ref[rows_of(g), cols] - crf * crf * gain
                    var_ref[rows_of(g), cols] = variance
                    total = total + variance
            colsum_ref[:, cols] = total

    pipelined(fill, work, (even_ref, odd_ref), ret_ref.shape[1] // wide)


def head_kernel(
    inv_ref, flip_ref, own_ref, other_ref, counts_own_ref, counts_other_ref, prior_own_ref, prior_other_ref,
    halo_ref, ret_ref, factor_ref, total_ref, crr_ref, colsum_ref, table_ref,
    var_ref, totals_ref, left_ref, even_ref, odd_ref, acc_ref,
):
    blocks = W // 8
    acc_ref[...] = jnp.zeros_like(acc_ref)
    for tile in range(SECTORS // LANES):
        mine = tile < HALF // LANES
        here, prior, counts = (
            (own_ref, prior_own_ref, counts_own_ref)
            if mine
            else (other_ref, prior_other_ref, counts_other_ref)
        )
        cols = pl.ds((tile * LANES) % HALF, LANES)
        scale = 1.0 / jnp.maximum(counts[W : W + 8, cols], 1.0)
        means = [
            (prior[rows_of(g), cols] if g < blocks else here[rows_of(g - blocks), cols]) * scale
            for g in range(2 * blocks)
        ]
        sector_rows(
            means, lambda g: inv_ref[rows_of(g)], 2 * blocks, (0, W, 2 * W), left_ref,
            tile * LANES, SECTORS, blocks,
        )
    row = lax.broadcasted_iota(jnp.int32, (8, LANES), 0)
    wide = even_ref.shape[1]

    def fill(buffer, index):
        cols = chunk_at(index, wide)
        buffer[...] = dot_nn(left_ref[...], twice(table_ref[:, cols]))

    def work(spread_ref, index):
        parts = []
        for tile in range(wide // LANES):
            inner = slice(tile * LANES, (tile + 1) * LANES)
            cols = pl.ds(pl.multiple_of(index * wide + tile * LANES, LANES), LANES)
            cross = Window()
            total = colsum_ref[:, cols]
            for group in range(2 * blocks):
                g = group - blocks
                if g < 0:
                    product = halo_ref[rows_of(group), cols] * spread_ref[rows_of(group), inner]
                else:
                    product = ret_ref[rows_of(g), cols] * factor_ref[rows_of(g), cols]
                product = cross.push(product, row)
                if g >= 0:
                    mean_f = spread_ref[rows_of(blocks + g), inner]
                    gain = spread_ref[rows_of(2 * blocks + g), inner]
                    crf = product - total_ref[rows_of(g), cols] * mean_f
                    variance = crr_ref[rows_of(g), cols] - crf * crf * gain
                    var_ref[rows_of(g), cols] = variance
                    total = total + variance
            hi = total.astype(bf16).astype(f32)
            mid = (total - hi).astype(bf16).astype(f32)
            parts.append(
                jnp.concatenate([hi, mid, total - hi - mid, jnp.zeros_like(hi)], axis=0).astype(bf16)
            )
        acc_ref[...] += dot_nt(
            jnp.concatenate(parts, axis=1), table_ref[:, chunk_at(index, wide)]
        )

    pipelined(fill, work, (even_ref, odd_ref), ret_ref.shape[1] // wide)
    total = jnp.sum(acc_ref[...], axis=0, keepdims=True)
    swapped = jnp.concatenate([total[:, HALF:], total[:, :HALF]], axis=1)
    total = jnp.where(flip_ref[0:1] == 0, total, swapped)
    totals_ref[...] = jnp.broadcast_to(total, totals_ref.shape)


VMEM = pl.BlockSpec(memory_space=pltpu.VMEM)


def kernel_call(body, outs, arrays, scratch=(), flops=0, moved=0):
    return kernel_of(body, outs, arrays, scratch, flops, moved)


def kernel_of(body, outs, arrays, scratch, flops, moved):
    return pl.pallas_call(
        body,
        out_shape=tuple(o if hasattr(o, "dtype") else jax.ShapeDtypeStruct(o, f32) for o in outs),
        in_specs=[VMEM] * len(arrays),
        out_specs=[VMEM] * len(outs),
        scratch_shapes=list(scratch),
        compiler_params=pltpu.CompilerParams(vmem_limit_bytes=10 * MIB),
        cost_estimate=pl.CostEstimate(flops=flops, bytes_accessed=moved, transcendentals=0),
    )(*arrays)


def shrink_kernel(
    all_steps, flip_ref, parts_ref, cown_ref, cother_ref, table_ref, head_ref, main_ref, out_hbm, out_ref, sems
):
    total = jnp.sum(parts_ref[...], axis=0, keepdims=True)
    swapped = jnp.concatenate([total[:, HALF:], total[:, :HALF]], axis=1)
    total = jnp.where(flip_ref[0:1] == 0, total, swapped)
    count = jnp.concatenate([cown_ref[W : W + 1], cother_ref[W : W + 1]], axis=1)
    mean = total / (all_steps * jnp.maximum(count, 1.0))
    left = split3_rows(shrink_weight / (1.0 - shrink_weight) * mean)
    chunks, _, wide = out_ref.shape
    copies = []
    for c in range(chunks):
        cols = slice(c * wide, (c + 1) * wide)
        pooled = jnp.sum(dot_nn(left, table_ref[:, cols]), axis=0, keepdims=True)
        out_ref[c, :W] = head_ref[:, cols] + pooled
        out_ref[c, W:] = main_ref[:, cols] + pooled
        copy = pltpu.make_async_copy(out_ref.at[c], out_hbm.at[:, pl.ds(c * wide, wide)], sems.at[c])
        copy.start()
        copies.append(copy)
    for copy in copies:
        copy.wait()


def shrink(all_steps, flip, parts, own, other, table, head, main):
    width = head.shape[1]
    rows = head.shape[0] + main.shape[0]
    chunks = 4
    return pl.pallas_call(
        functools.partial(shrink_kernel, float(all_steps)),
        out_shape=jax.ShapeDtypeStruct((rows, width), f32),
        in_specs=[VMEM] * 7,
        out_specs=pl.BlockSpec(memory_space=pltpu.HBM),
        scratch_shapes=[
            pltpu.VMEM((chunks, rows, width // chunks), f32),
            pltpu.SemaphoreType.DMA((chunks,)),
        ],
        compiler_params=pltpu.CompilerParams(vmem_limit_bytes=10 * MIB),
        cost_estimate=pl.CostEstimate(
            flops=2 * rows * width, bytes_accessed=8 * rows * width, transcendentals=0
        ),
        name="shrink",
    )(flip, parts, own, other, table, head, main)


def swap(value, axis, bit):
    return lax.ppermute(value, axis, [(i, i ^ bit) for i in range(lax.axis_size(axis))])


def ahead(value, axis):
    return lax.ppermute(value, axis, [(i, i + 1) for i in range(lax.axis_size(axis) - 1)])


def across(value, axis):
    bit = 2
    while bit < lax.axis_size(axis):
        value = value + swap(value, axis, bit)
        bit *= 2
    return value


def step(returns, sector):
    rows, width = returns.shape
    main = rows - W
    n_time, n_series = lax.axis_size("tm"), lax.axis_size("series")
    core = (lax.axis_index("series") % 2).astype(jnp.int32)
    first_step = (lax.axis_index("tm") * rows).astype(jnp.int32)
    wide = 4 * LANES
    hbm = pl.BlockSpec(memory_space=pltpu.HBM)
    keep, send, table, returns, tail, flip, inv = pl.pallas_call(
        load_kernel,
        out_shape=(
            jax.ShapeDtypeStruct((rows + 8, HALF), f32),
            jax.ShapeDtypeStruct((rows + 8, HALF), f32),
            jax.ShapeDtypeStruct((SECTORS, width), bf16),
            jax.ShapeDtypeStruct((rows, width), f32),
            jax.ShapeDtypeStruct((W, width), f32),
            jax.ShapeDtypeStruct((8, SECTORS), jnp.int32),
            jax.ShapeDtypeStruct((W, LANES), f32),
        ),
        in_specs=[hbm, hbm, VMEM, VMEM],
        out_specs=[VMEM] * 7,
        scratch_shapes=[
            pltpu.VMEM((1, width), jnp.int32),
            pltpu.VMEM((2 * rows + 32, wide), bf16),
            pltpu.VMEM((rows + 8, SECTORS), f32),
            pltpu.SemaphoreType.DMA,
            pltpu.SemaphoreType.DMA,
            pltpu.SemaphoreType.DMA((width // wide,)),
        ],
        compiler_params=pltpu.CompilerParams(vmem_limit_bytes=48 * MIB),
        name="load",
    )(
        returns,
        sector[None, :],
        jnp.broadcast_to(core, (8, LANES)),
        jnp.broadcast_to(first_step, (8, LANES)),
    )
    halo = ahead(tail, "tm")
    swapped = swap(send, "series", 1)
    own_tail = across(keep[main:] + swapped[main:], "series")
    own = across(keep[:main] + swapped[:main], "series")
    prior_own = ahead(own_tail, "tm")
    other_tail = swap(own_tail, "series", 1)
    other = swap(own, "series", 1)
    prior_other = swap(prior_own, "series", 1)
    chunk = 4 * LANES
    lhs = 3 * rows - 2 * W
    mean, crr = kernel_call(
        moments_main_kernel, [(main, width)] * 2, [returns],
        flops=40 * main * width, moved=12 * main * width,
    )
    mean_head, crr_head = kernel_call(
        moments_head_kernel, [(W, width)] * 2, [inv, halo, returns],
        flops=40 * W * width, moved=12 * W * width,
    )
    left = [pltpu.VMEM((lhs, SECTORS), bf16)]
    (spread,) = kernel_call(
        own_kernel, [(lhs, width)], [own, own_tail, table], scratch=left,
        flops=2 * lhs * width * SECTORS, moved=4 * lhs * width,
    )
    var, factor, colsum = kernel_call(
        main_kernel, [(main, width), (W, width), (8, width)],
        [other, other_tail, spread, returns, mean, crr, table],
        scratch=left + [pltpu.VMEM((lhs, chunk), f32)] * 2,
        flops=4 * lhs * width * SECTORS, moved=12 * rows * width,
    )
    var_head, totals = kernel_call(
        head_kernel, [(W, width), (n_time * n_series, SECTORS)],
        [inv, flip, own, other, own_tail, other_tail, prior_own, prior_other, halo, returns, factor,
         mean_head, crr_head, colsum, table],
        scratch=[pltpu.VMEM((3 * W, 2 * SECTORS), bf16)]
        + [pltpu.VMEM((3 * W, chunk), f32)] * 2
        + [pltpu.VMEM((32, SECTORS), f32)],
        flops=16 * W * width * SECTORS, moved=12 * W * width,
    )
    parts = lax.all_to_all(totals, ("tm", "series"), 0, 0)
    return shrink(n_time * rows, flip, parts, own_tail, other_tail, table, var_head, var)


def solution(mesh):
    placed = (P("tm", "series"), P("series"))
    return jax.shard_map(step, mesh=mesh, in_specs=placed, out_specs=P("tm", "series"), check_vma=False)
```

```python
import functools

import jax
import jax.numpy as jnp
from jax import lax
from jax.experimental import pallas as pl
from jax.experimental.pallas import tpu as pltpu
from jax.sharding import PartitionSpec as P


W = 64
SECTORS = 512
HALF = SECTORS // 2
LANES = 128

ridge_rate = 0.05
shrink_weight = 0.3

f32 = jnp.float32
bf16 = jnp.bfloat16
MIB = 1024 * 1024


def dot_nn(a, b):
    return lax.dot_general(a, b, (((1,), (0,)), ((), ())), preferred_element_type=f32)


def dot_nt(a, b):
    return lax.dot_general(a, b, (((1,), (1,)), ((), ())), preferred_element_type=f32)


def split2(x):
    hi = x.astype(bf16)
    return hi, (x - hi.astype(f32)).astype(bf16)


def split3_rows(x):
    hi = x.astype(bf16).astype(f32)
    rest = x - hi
    mid = rest.astype(bf16).astype(f32)
    low = rest - mid
    row = lax.broadcasted_iota(jnp.int32, (16, x.shape[1]), 0)
    return jnp.where(row == 0, hi, jnp.where(row == 1, mid, jnp.where(row == 2, low, 0.0))).astype(bf16)


def load_kernel(
    ret_hbm, sec_hbm, core_ref, first_ref,
    keep_ref, send_ref, table_ref, ret_ref, tail_ref, flip_ref, inv_ref,
    sec_ref, left_ref, acc_ref, sec_sem, tail_sem, ret_sems,
):
    rows, width = ret_ref.shape
    wide = left_ref.shape[1]
    height = rows + 16
    chunks = width // wide
    sec_copy = pltpu.make_async_copy(sec_hbm, sec_ref, sec_sem)
    sec_copy.start()
    copies = []
    for c in range(chunks):
        cols = pl.ds(c * wide, wide)
        copy = pltpu.make_async_copy(ret_hbm.at[:, cols], ret_ref.at[:, cols], ret_sems.at[c])
        copy.start()
        copies.append(copy)
    tail_copy = pltpu.make_async_copy(ret_hbm.at[pl.ds(rows - W, W)], tail_ref, tail_sem)
    tail_copy.start()
    flip_ref[...] = jnp.concatenate([core_ref[...]] * (SECTORS // LANES), axis=1)
    position = lax.broadcasted_iota(jnp.int32, (W, LANES), 0) + (first_ref[0:1] + 1)
    inv_ref[:W] = 1.0 / jnp.minimum(position, W).astype(f32)
    inv_ref[W:] = jnp.where(first_ref[...] > 0, 1.0, 0.0)
    left_ref[rows:height] = jnp.ones((16, wide), bf16)
    left_ref[height + rows :] = jnp.zeros((16, wide), bf16)
    turn = jnp.concatenate([core_ref[0:1] * HALF] * (wide // LANES), axis=1)
    sec_copy.wait()
    for c in range(chunks):
        cols = slice(c * wide, (c + 1) * wide)
        label = lax.broadcasted_iota(jnp.int32, (SECTORS, wide), 0)
        table_ref[:, cols] = jnp.where(label == (sec_ref[:, cols] ^ turn), 1.0, 0.0).astype(bf16)
    for c in range(chunks):
        cols = slice(c * wide, (c + 1) * wide)
        copies[c].wait()
        hi, lo = split2(ret_ref[:, cols])
        left_ref[:rows] = hi
        left_ref[height : height + rows] = lo
        part = dot_nt(left_ref[...], table_ref[:, cols])
        part = part[: rows + 8] + part[height : height + rows + 8]
        if c > 0:
            part = acc_ref[...] + part
        if c < chunks - 1:
            acc_ref[...] = part
    keep_ref[...] = part[:, :HALF]
    send_ref[...] = part[:, HALF:]
    tail_copy.wait()


class Window:
    def __init__(self):
        self.rolled = {}
        self.sums = {8: [], 16: [], 32: []}

    def push(self, x, row):
        size = 1
        while size < 8:
            turned = pltpu.roll(x, size, 0)
            before = self.rolled.get(size, turned)
            self.rolled[size] = turned
            x = x + jnp.where(row < size, before, turned)
            size *= 2
        while size < W:
            seen = self.sums[size]
            seen.append(x)
            back = size // 8
            if len(seen) <= back:
                return None
            x = x + seen[-1 - back]
            size *= 2
        return x


def tile_at(index):
    return pl.ds(pl.multiple_of(index * LANES, LANES), LANES)


def rows_of(group):
    return slice(group * 8, group * 8 + 8)


def moments_body(load, inv, groups, total_ref, crr_ref):
    row = lax.broadcasted_iota(jnp.int32, (8, LANES), 0)

    def tile(index, _):
        cols = tile_at(index)
        first, second = Window(), Window()
        for group in range(groups):
            ret = load(group, cols)
            total, squares = first.push(ret, row), second.push(ret * ret, row)
            if group >= W // 8:
                here = rows_of(group - W // 8)
                scale = inv(group - W // 8)
                mean = total * scale
                total_ref[here, cols] = total
                crr_ref[here, cols] = (1.0 - shrink_weight) * (squares * scale - mean * mean)
        return 0

    lax.fori_loop(0, total_ref.shape[1] // LANES, tile, 0)


def moments_main_kernel(ret_ref, mean_ref, crr_ref):
    moments_body(
        lambda group, cols: ret_ref[rows_of(group), cols],
        lambda group: 1.0 / W,
        ret_ref.shape[0] // 8,
        mean_ref,
        crr_ref,
    )


def moments_head_kernel(inv_ref, halo_ref, ret_ref, mean_ref, crr_ref):
    blocks = W // 8
    moments_body(
        lambda group, cols: halo_ref[rows_of(group), cols] * inv_ref[W:]
        if group < blocks
        else ret_ref[rows_of(group - blocks), cols],
        lambda group: inv_ref[rows_of(group)],
        2 * blocks,
        mean_ref,
        crr_ref,
    )


def sector_rows(means, inv, groups, starts, left_ref, out, low, kept=None):
    row = lax.broadcasted_iota(jnp.int32, (8, LANES), 0)
    first, second = Window(), Window()
    mean_parts, gain_parts = [], []
    for group in range(groups):
        mean = means[group]
        total, squares = first.push(mean, row), second.push(mean * mean, row)
        if group >= W // 8:
            scale = inv(group - W // 8)
            mean_f = total * scale
            spread = squares * scale - mean_f * mean_f + ridge_rate
            mean_parts.append(mean_f)
            gain_parts.append((1.0 - shrink_weight) * scale * scale / spread)
    for start, parts in zip(starts, (means[:kept], mean_parts, gain_parts)):
        for pair in range(0, len(parts), 2):
            hi, lo = split2(jnp.concatenate(parts[pair : pair + 2], axis=0))
            here = slice(start + pair * 8, start + pair * 8 + 16)
            left_ref[here, out : out + LANES] = hi
            left_ref[here, out + low : out + low + LANES] = lo


def pipelined(fill, work, buffers, chunks):
    even, odd = buffers
    fill(even, 0)

    def pair(j, _):
        fill(odd, 2 * j + 1)
        work(even, 2 * j)
        fill(even, 2 * j + 2)
        work(odd, 2 * j + 1)
        return 0

    lax.fori_loop(0, chunks // 2 - 1, pair, 0)
    fill(odd, chunks - 1)
    work(even, chunks - 2)
    work(odd, chunks - 1)


def chunk_at(index, wide):
    return pl.ds(pl.multiple_of(index * wide, wide), wide)


def main_rows(sums_ref, tail_ref, left_ref):
    main = sums_ref.shape[0]
    rows = main + W
    for tile in range(HALF // LANES):
        cols = slice(tile * LANES, (tile + 1) * LANES)
        scale = 1.0 / jnp.maximum(tail_ref[W : W + 8, cols], 1.0)
        means = [
            (sums_ref[rows_of(g), cols] if g < main // 8 else tail_ref[rows_of(g - main // 8), cols])
            * scale
            for g in range(rows // 8)
        ]
        sector_rows(
            means, lambda g: 1.0 / W, rows // 8, (0, rows, rows + main), left_ref, tile * LANES, HALF
        )


def twice(table):
    return jnp.concatenate([table, table], axis=0)


def own_kernel(own_ref, own_tail_ref, table_ref, spread_ref, left_ref):
    main_rows(own_ref, own_tail_ref, left_ref)
    wide = 4 * LANES
    for index in range(table_ref.shape[1] // wide):
        cols = slice(index * wide, (index + 1) * wide)
        spread_ref[:, cols] = dot_nn(left_ref[...], twice(table_ref[:HALF, cols]))


def main_kernel(
    other_ref, other_tail_ref, spread_ref, ret_ref, total_ref, crr_ref, table_ref,
    var_ref, factor_ref, colsum_ref, left_ref, even_ref, odd_ref,
):
    rows = ret_ref.shape[0]
    main = rows - W
    blocks = W // 8
    main_rows(other_ref, other_tail_ref, left_ref)
    row = lax.broadcasted_iota(jnp.int32, (8, LANES), 0)
    wide = even_ref.shape[1]

    def fill(buffer, index):
        cols = chunk_at(index, wide)
        buffer[...] = spread_ref[:, cols] + dot_nn(left_ref[...], twice(table_ref[HALF:, cols]))

    def work(spread_ref, index):
        for tile in range(wide // LANES):
            inner = slice(tile * LANES, (tile + 1) * LANES)
            cols = pl.ds(pl.multiple_of(index * wide + tile * LANES, LANES), LANES)
            cross = Window()
            total = jnp.zeros((8, LANES), f32)
            for group in range(rows // 8):
                factor = spread_ref[rows_of(group), inner]
                if group < blocks:
                    factor_ref[rows_of(group), cols] = factor
                product = cross.push(ret_ref[rows_of(group), cols] * factor, row)
                if group >= blocks:
                    g = group - blocks
                    mean_f = spread_ref[rows_of(rows // 8 + g), inner]
                    gain = spread_ref[rows_of((rows + main) // 8 + g), inner]
                    crf = product - total_ref[rows_of(g), cols] * mean_f
                    variance = crr_ref[rows_of(g), cols] - crf * crf * gain
                    var_ref[rows_of(g), cols] = variance
                    total = total + variance
            colsum_ref[:, cols] = total

    pipelined(fill, work, (even_ref, odd_ref), ret_ref.shape[1] // wide)


def head_kernel(
    inv_ref, flip_ref, own_ref, other_ref, counts_own_ref, counts_other_ref, prior_own_ref, prior_other_ref,
    halo_ref, ret_ref, factor_ref, total_ref, crr_ref, colsum_ref, table_ref,
    var_ref, totals_ref, left_ref, even_ref, odd_ref, acc_ref,
):
    blocks = W // 8
    acc_ref[...] = jnp.zeros_like(acc_ref)
    for tile in range(SECTORS // LANES):
        mine = tile < HALF // LANES
        here, prior, counts = (
            (own_ref, prior_own_ref, counts_own_ref)
            if mine
            else (other_ref, prior_other_ref, counts_other_ref)
        )
        cols = pl.ds((tile * LANES) % HALF, LANES)
        scale = 1.0 / jnp.maximum(counts[W : W + 8, cols], 1.0)
        means = [
            (prior[rows_of(g), cols] * inv_ref[W:] if g < blocks else here[rows_of(g - blocks), cols])
            * scale
            for g in range(2 * blocks)
        ]
        sector_rows(
            means, lambda g: inv_ref[rows_of(g)], 2 * blocks, (0, W, 2 * W), left_ref,
            tile * LANES, SECTORS, blocks,
        )
    row = lax.broadcasted_iota(jnp.int32, (8, LANES), 0)
    wide = even_ref.shape[1]

    def fill(buffer, index):
        cols = chunk_at(index, wide)
        buffer[...] = dot_nn(left_ref[...], twice(table_ref[:, cols]))

    def work(spread_ref, index):
        parts = []
        for tile in range(wide // LANES):
            inner = slice(tile * LANES, (tile + 1) * LANES)
            cols = pl.ds(pl.multiple_of(index * wide + tile * LANES, LANES), LANES)
            cross = Window()
            total = colsum_ref[:, cols]
            for group in range(2 * blocks):
                g = group - blocks
                if g < 0:
                    product = halo_ref[rows_of(group), cols] * spread_ref[rows_of(group), inner]
                    product = product * inv_ref[W:]
                else:
                    product = ret_ref[rows_of(g), cols] * factor_ref[rows_of(g), cols]
                product = cross.push(product, row)
                if g >= 0:
                    mean_f = spread_ref[rows_of(blocks + g), inner]
                    gain = spread_ref[rows_of(2 * blocks + g), inner]
                    crf = product - total_ref[rows_of(g), cols] * mean_f
                    variance = crr_ref[rows_of(g), cols] - crf * crf * gain
                    var_ref[rows_of(g), cols] = variance
                    total = total + variance
            hi = total.astype(bf16).astype(f32)
            mid = (total - hi).astype(bf16).astype(f32)
            parts.append(
                jnp.concatenate([hi, mid, total - hi - mid, jnp.zeros_like(hi)], axis=0).astype(bf16)
            )
        acc_ref[...] += dot_nt(
            jnp.concatenate(parts, axis=1), table_ref[:, chunk_at(index, wide)]
        )

    pipelined(fill, work, (even_ref, odd_ref), ret_ref.shape[1] // wide)
    total = jnp.sum(acc_ref[...], axis=0, keepdims=True)
    swapped = jnp.concatenate([total[:, HALF:], total[:, :HALF]], axis=1)
    total = jnp.where(flip_ref[0:1] == 0, total, swapped)
    totals_ref[...] = jnp.broadcast_to(total, totals_ref.shape)


VMEM = pl.BlockSpec(memory_space=pltpu.VMEM)


def kernel_call(body, outs, arrays, scratch=(), flops=0, moved=0):
    return kernel_of(body, outs, arrays, scratch, flops, moved)


def kernel_of(body, outs, arrays, scratch, flops, moved):
    return pl.pallas_call(
        body,
        out_shape=tuple(o if hasattr(o, "dtype") else jax.ShapeDtypeStruct(o, f32) for o in outs),
        in_specs=[VMEM] * len(arrays),
        out_specs=[VMEM] * len(outs),
        scratch_shapes=list(scratch),
        compiler_params=pltpu.CompilerParams(vmem_limit_bytes=10 * MIB),
        cost_estimate=pl.CostEstimate(flops=flops, bytes_accessed=moved, transcendentals=0),
    )(*arrays)


def shrink_kernel(
    all_steps, flip_ref, parts_ref, cown_ref, cother_ref, table_ref, head_ref, main_ref, out_hbm, out_ref, sems
):
    total = jnp.sum(parts_ref[...], axis=0, keepdims=True)
    swapped = jnp.concatenate([total[:, HALF:], total[:, :HALF]], axis=1)
    total = jnp.where(flip_ref[0:1] == 0, total, swapped)
    count = jnp.concatenate([cown_ref[W : W + 1], cother_ref[W : W + 1]], axis=1)
    mean = total / (all_steps * jnp.maximum(count, 1.0))
    left = split3_rows(shrink_weight / (1.0 - shrink_weight) * mean)
    chunks, _, wide = out_ref.shape
    copies = []
    for c in range(chunks):
        cols = slice(c * wide, (c + 1) * wide)
        pooled = jnp.sum(dot_nn(left, table_ref[:, cols]), axis=0, keepdims=True)
        out_ref[c, :W] = head_ref[:, cols] + pooled
        out_ref[c, W:] = main_ref[:, cols] + pooled
        copy = pltpu.make_async_copy(out_ref.at[c], out_hbm.at[:, pl.ds(c * wide, wide)], sems.at[c])
        copy.start()
        copies.append(copy)
    for copy in copies:
        copy.wait()


def shrink(all_steps, flip, parts, own, other, table, head, main):
    width = head.shape[1]
    rows = head.shape[0] + main.shape[0]
    chunks = 4
    return pl.pallas_call(
        functools.partial(shrink_kernel, float(all_steps)),
        out_shape=jax.ShapeDtypeStruct((rows, width), f32),
        in_specs=[VMEM] * 7,
        out_specs=pl.BlockSpec(memory_space=pltpu.HBM),
        scratch_shapes=[
            pltpu.VMEM((chunks, rows, width // chunks), f32),
            pltpu.SemaphoreType.DMA((chunks,)),
        ],
        compiler_params=pltpu.CompilerParams(vmem_limit_bytes=10 * MIB),
        cost_estimate=pl.CostEstimate(
            flops=2 * rows * width, bytes_accessed=8 * rows * width, transcendentals=0
        ),
        name="shrink",
    )(flip, parts, own, other, table, head, main)


def swap(value, axis, bit):
    return lax.ppermute(value, axis, [(i, i ^ bit) for i in range(lax.axis_size(axis))])


def ahead(value, axis):
    count = lax.axis_size(axis)
    return lax.ppermute(value, axis, [(i, (i + 1) % count) for i in range(count)])


def across(value, axis):
    bit = 2
    while bit < lax.axis_size(axis):
        value = value + swap(value, axis, bit)
        bit *= 2
    return value


def step(returns, sector):
    rows, width = returns.shape
    main = rows - W
    n_time, n_series = lax.axis_size("tm"), lax.axis_size("series")
    core = (lax.axis_index("series") % 2).astype(jnp.int32)
    first_step = (lax.axis_index("tm") * rows).astype(jnp.int32)
    wide = 4 * LANES
    hbm = pl.BlockSpec(memory_space=pltpu.HBM)
    keep, send, table, returns, tail, flip, inv = pl.pallas_call(
        load_kernel,
        out_shape=(
            jax.ShapeDtypeStruct((rows + 8, HALF), f32),
            jax.ShapeDtypeStruct((rows + 8, HALF), f32),
            jax.ShapeDtypeStruct((SECTORS, width), bf16),
            jax.ShapeDtypeStruct((rows, width), f32),
            jax.ShapeDtypeStruct((W, width), f32),
            jax.ShapeDtypeStruct((8, SECTORS), jnp.int32),
            jax.ShapeDtypeStruct((W + 8, LANES), f32),
        ),
        in_specs=[hbm, hbm, VMEM, VMEM],
        out_specs=[VMEM] * 7,
        scratch_shapes=[
            pltpu.VMEM((1, width), jnp.int32),
            pltpu.VMEM((2 * rows + 32, wide), bf16),
            pltpu.VMEM((rows + 8, SECTORS), f32),
            pltpu.SemaphoreType.DMA,
            pltpu.SemaphoreType.DMA,
            pltpu.SemaphoreType.DMA((width // wide,)),
        ],
        compiler_params=pltpu.CompilerParams(vmem_limit_bytes=48 * MIB),
        name="load",
    )(
        returns,
        sector[None, :],
        jnp.broadcast_to(core, (8, LANES)),
        jnp.broadcast_to(first_step, (8, LANES)),
    )
    halo = ahead(tail, "tm")
    swapped = swap(send, "series", 1)
    own_tail = across(keep[main:] + swapped[main:], "series")
    own = across(keep[:main] + swapped[:main], "series")
    prior_own = ahead(own_tail[:W], "tm")
    other_tail = swap(own_tail, "series", 1)
    other = swap(own, "series", 1)
    prior_other = swap(prior_own, "series", 1)
    chunk = 4 * LANES
    lhs = 3 * rows - 2 * W
    mean, crr = kernel_call(
        moments_main_kernel, [(main, width)] * 2, [returns],
        flops=40 * main * width, moved=12 * main * width,
    )
    mean_head, crr_head = kernel_call(
        moments_head_kernel, [(W, width)] * 2, [inv, halo, returns],
        flops=40 * W * width, moved=12 * W * width,
    )
    left = [pltpu.VMEM((lhs, SECTORS), bf16)]
    (spread,) = kernel_call(
        own_kernel, [(lhs, width)], [own, own_tail, table], scratch=left,
        flops=2 * lhs * width * SECTORS, moved=4 * lhs * width,
    )
    var, factor, colsum = kernel_call(
        main_kernel, [(main, width), (W, width), (8, width)],
        [other, other_tail, spread, returns, mean, crr, table],
        scratch=left + [pltpu.VMEM((lhs, chunk), f32)] * 2,
        flops=4 * lhs * width * SECTORS, moved=12 * rows * width,
    )
    var_head, totals = kernel_call(
        head_kernel, [(W, width), (n_time * n_series, SECTORS)],
        [inv, flip, own, other, own_tail, other_tail, prior_own, prior_other, halo, returns, factor,
         mean_head, crr_head, colsum, table],
        scratch=[pltpu.VMEM((3 * W, 2 * SECTORS), bf16)]
        + [pltpu.VMEM((3 * W, chunk), f32)] * 2
        + [pltpu.VMEM((32, SECTORS), f32)],
        flops=16 * W * width * SECTORS, moved=12 * W * width,
    )
    parts = lax.all_to_all(totals, ("tm", "series"), 0, 0)
    return shrink(n_time * rows, flip, parts, own_tail, other_tail, table, var_head, var)


def solution(mesh):
    placed = (P("tm", "series"), P("series"))
    return jax.shard_map(step, mesh=mesh, in_specs=placed, out_specs=P("tm", "series"), check_vma=False)
```

```python
import functools

import jax
import jax.numpy as jnp
from jax import lax
from jax.experimental import pallas as pl
from jax.experimental.pallas import tpu as pltpu
from jax.sharding import PartitionSpec as P


W = 64
SECTORS = 512
HALF = SECTORS // 2
LANES = 128

ridge_rate = 0.05
shrink_weight = 0.3

f32 = jnp.float32
bf16 = jnp.bfloat16
MIB = 1024 * 1024


def dot_nn(a, b):
    return lax.dot_general(a, b, (((1,), (0,)), ((), ())), preferred_element_type=f32)


def dot_nt(a, b):
    return lax.dot_general(a, b, (((1,), (1,)), ((), ())), preferred_element_type=f32)


def split2(x):
    hi = x.astype(bf16)
    return hi, (x - hi.astype(f32)).astype(bf16)


def split3_rows(x):
    hi = x.astype(bf16).astype(f32)
    rest = x - hi
    mid = rest.astype(bf16).astype(f32)
    low = rest - mid
    row = lax.broadcasted_iota(jnp.int32, (16, x.shape[1]), 0)
    return jnp.where(row == 0, hi, jnp.where(row == 1, mid, jnp.where(row == 2, low, 0.0))).astype(bf16)


def load_kernel(
    ret_hbm, sec_hbm, core_ref, first_ref,
    keep_ref, send_ref, table_ref, ret_ref, tail_ref, flip_ref, inv_ref,
    sec_ref, left_ref, acc_ref, sec_sem, tail_sem, ret_sems,
):
    rows, width = ret_ref.shape
    wide = left_ref.shape[1]
    height = rows + 16
    chunks = width // wide
    sec_copy = pltpu.make_async_copy(sec_hbm, sec_ref, sec_sem)
    sec_copy.start()
    copies = []
    for c in range(chunks):
        cols = pl.ds(c * wide, wide)
        copy = pltpu.make_async_copy(ret_hbm.at[:, cols], ret_ref.at[:, cols], ret_sems.at[c])
        copy.start()
        copies.append(copy)
    tail_copy = pltpu.make_async_copy(ret_hbm.at[pl.ds(rows - W, W)], tail_ref, tail_sem)
    tail_copy.start()
    flip_ref[...] = jnp.concatenate([core_ref[...]] * (SECTORS // LANES), axis=1)
    position = lax.broadcasted_iota(jnp.int32, (W, LANES), 0) + (first_ref[0:1] + 1)
    inv_ref[:W] = 1.0 / jnp.minimum(position, W).astype(f32)
    inv_ref[W:] = jnp.where(first_ref[...] > 0, 1.0, 0.0)
    left_ref[rows:height] = jnp.ones((16, wide), bf16)
    left_ref[height + rows :] = jnp.zeros((16, wide), bf16)
    turn = jnp.concatenate([core_ref[0:1] * HALF] * (wide // LANES), axis=1)
    sec_copy.wait()
    for c in range(chunks):
        cols = slice(c * wide, (c + 1) * wide)
        label = lax.broadcasted_iota(jnp.int32, (SECTORS, wide), 0)
        table_ref[:, cols] = jnp.where(label == (sec_ref[:, cols] ^ turn), 1.0, 0.0).astype(bf16)
    for c in range(chunks):
        cols = slice(c * wide, (c + 1) * wide)
        copies[c].wait()
        hi, lo = split2(ret_ref[:, cols])
        left_ref[:rows] = hi
        left_ref[height : height + rows] = lo
        part = dot_nt(left_ref[...], table_ref[:, cols])
        part = part[: rows + 8] + part[height : height + rows + 8]
        if c > 0:
            part = acc_ref[...] + part
        if c < chunks - 1:
            acc_ref[...] = part
    keep_ref[...] = part[:, :HALF]
    send_ref[...] = part[:, HALF:]
    tail_copy.wait()


class Window:
    def __init__(self):
        self.rolled = {}
        self.sums = {8: [], 16: [], 32: []}

    def push(self, x, row):
        size = 1
        while size < 8:
            turned = pltpu.roll(x, size, 0)
            before = self.rolled.get(size, turned)
            self.rolled[size] = turned
            x = x + jnp.where(row < size, before, turned)
            size *= 2
        while size < W:
            seen = self.sums[size]
            seen.append(x)
            back = size // 8
            if len(seen) <= back:
                return None
            x = x + seen[-1 - back]
            size *= 2
        return x


def tile_at(index):
    return pl.ds(pl.multiple_of(index * LANES, LANES), LANES)


def rows_of(group):
    return slice(group * 8, group * 8 + 8)


def moments_body(load, inv, groups, total_ref, crr_ref):
    row = lax.broadcasted_iota(jnp.int32, (8, LANES), 0)

    def tile(index, _):
        cols = tile_at(index)
        first, second = Window(), Window()
        for group in range(groups):
            ret = load(group, cols)
            total, squares = first.push(ret, row), second.push(ret * ret, row)
            if group >= W // 8:
                here = rows_of(group - W // 8)
                scale = inv(group - W // 8)
                mean = total * scale
                total_ref[here, cols] = total
                crr_ref[here, cols] = (1.0 - shrink_weight) * (squares * scale - mean * mean)
        return 0

    lax.fori_loop(0, total_ref.shape[1] // LANES, tile, 0)


def moments_main_kernel(ret_ref, mean_ref, crr_ref):
    moments_body(
        lambda group, cols: ret_ref[rows_of(group), cols],
        lambda group: 1.0 / W,
        ret_ref.shape[0] // 8,
        mean_ref,
        crr_ref,
    )


def moments_head_kernel(inv_ref, halo_ref, ret_ref, mean_ref, crr_ref):
    blocks = W // 8
    moments_body(
        lambda group, cols: halo_ref[rows_of(group), cols] * inv_ref[W:]
        if group < blocks
        else ret_ref[rows_of(group - blocks), cols],
        lambda group: inv_ref[rows_of(group)],
        2 * blocks,
        mean_ref,
        crr_ref,
    )


def sector_rows(means, inv, groups, starts, left_ref, out, low, kept=slice(None)):
    row = lax.broadcasted_iota(jnp.int32, (8, LANES), 0)
    first, second = Window(), Window()
    mean_parts, gain_parts = [], []
    for group in range(groups):
        mean = means[group]
        total, squares = first.push(mean, row), second.push(mean * mean, row)
        if group >= W // 8:
            scale = inv(group - W // 8)
            mean_f = total * scale
            spread = squares * scale - mean_f * mean_f + ridge_rate
            mean_parts.append(mean_f)
            gain_parts.append((1.0 - shrink_weight) * scale * scale / spread)
    for start, parts in zip(starts, (means[kept], mean_parts, gain_parts)):
        for pair in range(0, len(parts), 2):
            hi, lo = split2(jnp.concatenate(parts[pair : pair + 2], axis=0))
            here = slice(start + pair * 8, start + pair * 8 + 16)
            left_ref[here, out : out + LANES] = hi
            left_ref[here, out + low : out + low + LANES] = lo


def pipelined(fill, work, buffers, chunks):
    even, odd = buffers
    fill(even, 0)

    def pair(j, _):
        fill(odd, 2 * j + 1)
        work(even, 2 * j)
        fill(even, 2 * j + 2)
        work(odd, 2 * j + 1)
        return 0

    lax.fori_loop(0, chunks // 2 - 1, pair, 0)
    fill(odd, chunks - 1)
    work(even, chunks - 2)
    work(odd, chunks - 1)


def chunk_at(index, wide):
    return pl.ds(pl.multiple_of(index * wide, wide), wide)


def early_rows(early_ref, tail_ref, left_ref):
    rows = early_ref.shape[0]
    for tile in range(HALF // LANES):
        cols = slice(tile * LANES, (tile + 1) * LANES)
        scale = 1.0 / jnp.maximum(tail_ref[W : W + 8, cols], 1.0)
        means = [early_ref[rows_of(g), cols] * scale for g in range(rows // 8)]
        starts = (0, rows, 2 * rows - W)
        sector_rows(means, lambda g: 1.0 / W, rows // 8, starts, left_ref, tile * LANES, HALF)


def late_rows(early_ref, late_ref, tail_ref, left_ref, base):
    before, middle = early_ref.shape[0], late_ref.shape[0]
    rows = middle + W
    for tile in range(HALF // LANES):
        cols = slice(tile * LANES, (tile + 1) * LANES)
        scale = 1.0 / jnp.maximum(tail_ref[W : W + 8, cols], 1.0)
        sums = [early_ref[rows_of(g), cols] for g in range((before - W) // 8, before // 8)]
        sums += [late_ref[rows_of(g), cols] for g in range(middle // 8)]
        sums += [tail_ref[rows_of(g), cols] for g in range(W // 8)]
        starts = (base, base + rows, base + 2 * rows)
        sector_rows(
            [part * scale for part in sums], lambda g: 1.0 / W, len(sums), starts, left_ref,
            tile * LANES, HALF, slice(W // 8, None),
        )


def twice(table):
    return jnp.concatenate([table, table], axis=0)


def spread_half(left_ref, table_ref, spread_ref):
    wide = 4 * LANES
    for index in range(table_ref.shape[1] // wide):
        cols = slice(index * wide, (index + 1) * wide)
        spread_ref[:, cols] = dot_nn(left_ref[...], twice(table_ref[:HALF, cols]))


def own_early_kernel(early_ref, tail_ref, table_ref, spread_ref, left_ref):
    early_rows(early_ref, tail_ref, left_ref)
    spread_half(left_ref, table_ref, spread_ref)


def own_late_kernel(early_ref, late_ref, tail_ref, table_ref, spread_ref, left_ref):
    late_rows(early_ref, late_ref, tail_ref, left_ref, 0)
    spread_half(left_ref, table_ref, spread_ref)


def main_kernel(
    early_ref, late_ref, tail_ref, spread_early_ref, spread_late_ref, ret_ref, total_ref, crr_ref, table_ref,
    var_ref, factor_ref, colsum_ref, left_ref, even_ref, odd_ref,
):
    rows = ret_ref.shape[0]
    blocks = W // 8
    base = spread_early_ref.shape[0]
    early = early_ref.shape[0] // 8
    late = rows // 8 - early
    opening = early - blocks

    def factor_at(group):
        return rows_of(group if group < early else base // 8 + group - early)

    def mean_at(g):
        return rows_of(early + g if g < opening else base // 8 + late + g - opening)

    def gain_at(g):
        return rows_of(early + opening + g if g < opening else base // 8 + 2 * late + g - opening)

    early_rows(early_ref, tail_ref, left_ref)
    late_rows(early_ref, late_ref, tail_ref, left_ref, base)
    row = lax.broadcasted_iota(jnp.int32, (8, LANES), 0)
    wide = even_ref.shape[1]

    def fill(buffer, index):
        cols = chunk_at(index, wide)
        other = dot_nn(left_ref[...], twice(table_ref[HALF:, cols]))
        buffer[:base] = spread_early_ref[:, cols] + other[:base]
        buffer[base:] = spread_late_ref[:, cols] + other[base:]

    def work(spread_ref, index):
        for tile in range(wide // LANES):
            inner = slice(tile * LANES, (tile + 1) * LANES)
            cols = pl.ds(pl.multiple_of(index * wide + tile * LANES, LANES), LANES)
            cross = Window()
            total = jnp.zeros((8, LANES), f32)
            for group in range(rows // 8):
                factor = spread_ref[factor_at(group), inner]
                if group < blocks:
                    factor_ref[rows_of(group), cols] = factor
                product = cross.push(ret_ref[rows_of(group), cols] * factor, row)
                if group >= blocks:
                    g = group - blocks
                    mean_f = spread_ref[mean_at(g), inner]
                    gain = spread_ref[gain_at(g), inner]
                    crf = product - total_ref[rows_of(g), cols] * mean_f
                    variance = crr_ref[rows_of(g), cols] - crf * crf * gain
                    var_ref[rows_of(g), cols] = variance
                    total = total + variance
            colsum_ref[:, cols] = total

    pipelined(fill, work, (even_ref, odd_ref), ret_ref.shape[1] // wide)


def head_kernel(
    inv_ref, flip_ref, own_ref, other_ref, counts_own_ref, counts_other_ref, prior_own_ref, prior_other_ref,
    halo_ref, ret_ref, factor_ref, total_ref, crr_ref, colsum_ref, table_ref,
    var_ref, totals_ref, left_ref, even_ref, odd_ref, acc_ref,
):
    blocks = W // 8
    acc_ref[...] = jnp.zeros_like(acc_ref)
    for tile in range(SECTORS // LANES):
        mine = tile < HALF // LANES
        here, prior, counts = (
            (own_ref, prior_own_ref, counts_own_ref)
            if mine
            else (other_ref, prior_other_ref, counts_other_ref)
        )
        cols = pl.ds((tile * LANES) % HALF, LANES)
        scale = 1.0 / jnp.maximum(counts[W : W + 8, cols], 1.0)
        means = [
            (prior[rows_of(g), cols] * inv_ref[W:] if g < blocks else here[rows_of(g - blocks), cols])
            * scale
            for g in range(2 * blocks)
        ]
        sector_rows(
            means, lambda g: inv_ref[rows_of(g)], 2 * blocks, (0, W, 2 * W), left_ref,
            tile * LANES, SECTORS, slice(blocks),
        )
    row = lax.broadcasted_iota(jnp.int32, (8, LANES), 0)
    wide = even_ref.shape[1]

    def fill(buffer, index):
        cols = chunk_at(index, wide)
        buffer[...] = dot_nn(left_ref[...], twice(table_ref[:, cols]))

    def work(spread_ref, index):
        parts = []
        for tile in range(wide // LANES):
            inner = slice(tile * LANES, (tile + 1) * LANES)
            cols = pl.ds(pl.multiple_of(index * wide + tile * LANES, LANES), LANES)
            cross = Window()
            total = colsum_ref[:, cols]
            for group in range(2 * blocks):
                g = group - blocks
                if g < 0:
                    product = halo_ref[rows_of(group), cols] * spread_ref[rows_of(group), inner]
                    product = product * inv_ref[W:]
                else:
                    product = ret_ref[rows_of(g), cols] * factor_ref[rows_of(g), cols]
                product = cross.push(product, row)
                if g >= 0:
                    mean_f = spread_ref[rows_of(blocks + g), inner]
                    gain = spread_ref[rows_of(2 * blocks + g), inner]
                    crf = product - total_ref[rows_of(g), cols] * mean_f
                    variance = crr_ref[rows_of(g), cols] - crf * crf * gain
                    var_ref[rows_of(g), cols] = variance
                    total = total + variance
            hi = total.astype(bf16).astype(f32)
            mid = (total - hi).astype(bf16).astype(f32)
            parts.append(
                jnp.concatenate([hi, mid, total - hi - mid, jnp.zeros_like(hi)], axis=0).astype(bf16)
            )
        acc_ref[...] += dot_nt(
            jnp.concatenate(parts, axis=1), table_ref[:, chunk_at(index, wide)]
        )

    pipelined(fill, work, (even_ref, odd_ref), ret_ref.shape[1] // wide)
    total = jnp.sum(acc_ref[...], axis=0, keepdims=True)
    swapped = jnp.concatenate([total[:, HALF:], total[:, :HALF]], axis=1)
    total = jnp.where(flip_ref[0:1] == 0, total, swapped)
    totals_ref[...] = jnp.broadcast_to(total, totals_ref.shape)


VMEM = pl.BlockSpec(memory_space=pltpu.VMEM)


def kernel_call(body, outs, arrays, scratch=(), flops=0, moved=0):
    return kernel_of(body, outs, arrays, scratch, flops, moved)


def kernel_of(body, outs, arrays, scratch, flops, moved):
    return pl.pallas_call(
        body,
        out_shape=tuple(o if hasattr(o, "dtype") else jax.ShapeDtypeStruct(o, f32) for o in outs),
        in_specs=[VMEM] * len(arrays),
        out_specs=[VMEM] * len(outs),
        scratch_shapes=list(scratch),
        compiler_params=pltpu.CompilerParams(vmem_limit_bytes=10 * MIB),
        cost_estimate=pl.CostEstimate(flops=flops, bytes_accessed=moved, transcendentals=0),
    )(*arrays)


def shrink_kernel(
    all_steps, flip_ref, parts_ref, cown_ref, cother_ref, table_ref, head_ref, main_ref, out_hbm, out_ref, sems
):
    total = jnp.sum(parts_ref[...], axis=0, keepdims=True)
    swapped = jnp.concatenate([total[:, HALF:], total[:, :HALF]], axis=1)
    total = jnp.where(flip_ref[0:1] == 0, total, swapped)
    count = jnp.concatenate([cown_ref[W : W + 1], cother_ref[W : W + 1]], axis=1)
    mean = total / (all_steps * jnp.maximum(count, 1.0))
    left = split3_rows(shrink_weight / (1.0 - shrink_weight) * mean)
    chunks, _, wide = out_ref.shape
    copies = []
    for c in range(chunks):
        cols = slice(c * wide, (c + 1) * wide)
        pooled = jnp.sum(dot_nn(left, table_ref[:, cols]), axis=0, keepdims=True)
        out_ref[c, :W] = head_ref[:, cols] + pooled
        out_ref[c, W:] = main_ref[:, cols] + pooled
        copy = pltpu.make_async_copy(out_ref.at[c], out_hbm.at[:, pl.ds(c * wide, wide)], sems.at[c])
        copy.start()
        copies.append(copy)
    for copy in copies:
        copy.wait()


def shrink(all_steps, flip, parts, own, other, table, head, main):
    width = head.shape[1]
    rows = head.shape[0] + main.shape[0]
    chunks = 4
    return pl.pallas_call(
        functools.partial(shrink_kernel, float(all_steps)),
        out_shape=jax.ShapeDtypeStruct((rows, width), f32),
        in_specs=[VMEM] * 7,
        out_specs=pl.BlockSpec(memory_space=pltpu.HBM),
        scratch_shapes=[
            pltpu.VMEM((chunks, rows, width // chunks), f32),
            pltpu.SemaphoreType.DMA((chunks,)),
        ],
        compiler_params=pltpu.CompilerParams(vmem_limit_bytes=10 * MIB),
        cost_estimate=pl.CostEstimate(
            flops=2 * rows * width, bytes_accessed=8 * rows * width, transcendentals=0
        ),
        name="shrink",
    )(flip, parts, own, other, table, head, main)


def swap(value, axis, bit):
    return lax.ppermute(value, axis, [(i, i ^ bit) for i in range(lax.axis_size(axis))])


def ahead(value, axis):
    count = lax.axis_size(axis)
    return lax.ppermute(value, axis, [(i, (i + 1) % count) for i in range(count)])


def across(value, axis):
    bit = 2
    while bit < lax.axis_size(axis):
        value = value + swap(value, axis, bit)
        bit *= 2
    return value


def step(returns, sector):
    rows, width = returns.shape
    main = rows - W
    n_time, n_series = lax.axis_size("tm"), lax.axis_size("series")
    core = (lax.axis_index("series") % 2).astype(jnp.int32)
    first_step = (lax.axis_index("tm") * rows).astype(jnp.int32)
    wide = 4 * LANES
    hbm = pl.BlockSpec(memory_space=pltpu.HBM)
    keep, send, table, returns, tail, flip, inv = pl.pallas_call(
        load_kernel,
        out_shape=(
            jax.ShapeDtypeStruct((rows + 8, HALF), f32),
            jax.ShapeDtypeStruct((rows + 8, HALF), f32),
            jax.ShapeDtypeStruct((SECTORS, width), bf16),
            jax.ShapeDtypeStruct((rows, width), f32),
            jax.ShapeDtypeStruct((W, width), f32),
            jax.ShapeDtypeStruct((8, SECTORS), jnp.int32),
            jax.ShapeDtypeStruct((W + 8, LANES), f32),
        ),
        in_specs=[hbm, hbm, VMEM, VMEM],
        out_specs=[VMEM] * 7,
        scratch_shapes=[
            pltpu.VMEM((1, width), jnp.int32),
            pltpu.VMEM((2 * rows + 32, wide), bf16),
            pltpu.VMEM((rows + 8, SECTORS), f32),
            pltpu.SemaphoreType.DMA,
            pltpu.SemaphoreType.DMA,
            pltpu.SemaphoreType.DMA((width // wide,)),
        ],
        compiler_params=pltpu.CompilerParams(vmem_limit_bytes=48 * MIB),
        name="load",
    )(
        returns,
        sector[None, :],
        jnp.broadcast_to(core, (8, LANES)),
        jnp.broadcast_to(first_step, (8, LANES)),
    )
    halo = ahead(tail, "tm")
    swapped = swap(send, "series", 1)
    own_tail = across(keep[main:] + swapped[main:], "series")
    half = rows // 2
    early = across(keep[:half] + swapped[:half], "series")
    late = across(keep[half:main] + swapped[half:main], "series")
    prior_own = ahead(own_tail[:W], "tm")
    other_tail = swap(own_tail, "series", 1)
    other_early = swap(early, "series", 1)
    other_late = swap(late, "series", 1)
    prior_other = swap(prior_own, "series", 1)
    chunk = 4 * LANES
    lhs_early, lhs_late = 3 * half - 2 * W, 3 * half
    mean, crr = kernel_call(
        moments_main_kernel, [(main, width)] * 2, [returns],
        flops=40 * main * width, moved=12 * main * width,
    )
    mean_head, crr_head = kernel_call(
        moments_head_kernel, [(W, width)] * 2, [inv, halo, returns],
        flops=40 * W * width, moved=12 * W * width,
    )
    (spread_early,) = kernel_call(
        own_early_kernel, [(lhs_early, width)], [early, own_tail, table],
        scratch=[pltpu.VMEM((lhs_early, SECTORS), bf16)],
        flops=2 * lhs_early * width * SECTORS, moved=4 * lhs_early * width,
    )
    (spread_late,) = kernel_call(
        own_late_kernel, [(lhs_late, width)], [early, late, own_tail, table],
        scratch=[pltpu.VMEM((lhs_late, SECTORS), bf16)],
        flops=2 * lhs_late * width * SECTORS, moved=4 * lhs_late * width,
    )
    lhs = lhs_early + lhs_late
    var, factor, colsum = kernel_call(
        main_kernel, [(main, width), (W, width), (8, width)],
        [other_early, other_late, other_tail, spread_early, spread_late, returns, mean, crr, table],
        scratch=[pltpu.VMEM((lhs, SECTORS), bf16)] + [pltpu.VMEM((lhs, chunk), f32)] * 2,
        flops=4 * lhs * width * SECTORS, moved=12 * rows * width,
    )
    var_head, totals = kernel_call(
        head_kernel, [(W, width), (n_time * n_series, SECTORS)],
        [inv, flip, early, other_early, own_tail, other_tail, prior_own, prior_other, halo, returns, factor,
         mean_head, crr_head, colsum, table],
        scratch=[pltpu.VMEM((3 * W, 2 * SECTORS), bf16)]
        + [pltpu.VMEM((3 * W, chunk), f32)] * 2
        + [pltpu.VMEM((32, SECTORS), f32)],
        flops=16 * W * width * SECTORS, moved=12 * W * width,
    )
    parts = lax.all_to_all(totals, ("tm", "series"), 0, 0)
    return shrink(n_time * rows, flip, parts, own_tail, other_tail, table, var_head, var)


def solution(mesh):
    placed = (P("tm", "series"), P("series"))
    return jax.shard_map(step, mesh=mesh, in_specs=placed, out_specs=P("tm", "series"), check_vma=False)
```

```python
import functools

import jax
import jax.numpy as jnp
from jax import lax
from jax.experimental import pallas as pl
from jax.experimental.pallas import tpu as pltpu
from jax.sharding import PartitionSpec as P


W = 64
SECTORS = 512
HALF = SECTORS // 2
LANES = 128

ridge_rate = 0.05
shrink_weight = 0.3

f32 = jnp.float32
bf16 = jnp.bfloat16
MIB = 1024 * 1024


def dot_nn(a, b):
    return lax.dot_general(a, b, (((1,), (0,)), ((), ())), preferred_element_type=f32)


def dot_nt(a, b):
    return lax.dot_general(a, b, (((1,), (1,)), ((), ())), preferred_element_type=f32)


def split2(x):
    hi = x.astype(bf16)
    return hi, (x - hi.astype(f32)).astype(bf16)


def split3_rows(x):
    hi = x.astype(bf16).astype(f32)
    rest = x - hi
    mid = rest.astype(bf16).astype(f32)
    low = rest - mid
    row = lax.broadcasted_iota(jnp.int32, (16, x.shape[1]), 0)
    return jnp.where(row == 0, hi, jnp.where(row == 1, mid, jnp.where(row == 2, low, 0.0))).astype(bf16)


def load_kernel(
    ret_hbm, sec_hbm, core_ref, first_ref,
    keep_ref, send_ref, table_ref, ret_ref, tail_ref, flip_ref, inv_ref,
    sec_ref, left_ref, acc_ref, sec_sem, tail_sem, ret_sems,
):
    rows, width = ret_ref.shape
    wide = left_ref.shape[1]
    height = rows + 16
    chunks = width // wide
    sec_copy = pltpu.make_async_copy(sec_hbm, sec_ref, sec_sem)
    sec_copy.start()
    copies = []
    for c in range(chunks):
        cols = pl.ds(c * wide, wide)
        copy = pltpu.make_async_copy(ret_hbm.at[:, cols], ret_ref.at[:, cols], ret_sems.at[c])
        copy.start()
        copies.append(copy)
    tail_copy = pltpu.make_async_copy(ret_hbm.at[pl.ds(rows - W, W)], tail_ref, tail_sem)
    tail_copy.start()
    flip_ref[...] = jnp.concatenate([core_ref[...]] * (SECTORS // LANES), axis=1)
    position = lax.broadcasted_iota(jnp.int32, (W, LANES), 0) + (first_ref[0:1] + 1)
    inv_ref[:W] = 1.0 / jnp.minimum(position, W).astype(f32)
    inv_ref[W:] = jnp.where(first_ref[...] > 0, 1.0, 0.0)
    left_ref[rows:height] = jnp.ones((16, wide), bf16)
    left_ref[height + rows :] = jnp.zeros((16, wide), bf16)
    turn = jnp.concatenate([core_ref[0:1] * HALF] * (wide // LANES), axis=1)
    sec_copy.wait()
    for c in range(chunks):
        cols = slice(c * wide, (c + 1) * wide)
        label = lax.broadcasted_iota(jnp.int32, (SECTORS, wide), 0)
        table_ref[:, cols] = jnp.where(label == (sec_ref[:, cols] ^ turn), 1.0, 0.0).astype(bf16)
    for c in range(chunks):
        cols = slice(c * wide, (c + 1) * wide)
        copies[c].wait()
        hi, lo = split2(ret_ref[:, cols])
        left_ref[:rows] = hi
        left_ref[height : height + rows] = lo
        part = dot_nt(left_ref[...], table_ref[:, cols])
        part = part[: rows + 8] + part[height : height + rows + 8]
        if c > 0:
            part = acc_ref[...] + part
        if c < chunks - 1:
            acc_ref[...] = part
    keep_ref[...] = part[:, :HALF]
    send_ref[...] = part[:, HALF:]
    tail_copy.wait()


SHIFTED = (1, 2, 4)


class Window:
    def __init__(self, ref, row):
        self.ref, self.row, self.groups = ref, row, 0
        self.rolled = {}
        self.sums = {8: [], 16: [], 32: []}

    def push(self, x):
        here = 8 + 8 * self.groups
        self.groups += 1
        size = 1
        while size < 8:
            if size in SHIFTED:
                slot = SHIFTED.index(size)
                self.ref[slot, here : here + 8] = x
                x = x + self.ref[slot, here - size : here - size + 8]
            else:
                turned = pltpu.roll(x, size, 0)
                before = self.rolled.get(size, turned)
                self.rolled[size] = turned
                x = x + jnp.where(self.row < size, before, turned)
            size *= 2
        while size < W:
            seen = self.sums[size]
            seen.append(x)
            back = size // 8
            if len(seen) <= back:
                return None
            x = x + seen[-1 - back]
            size *= 2
        return x


def stage(count, rows):
    return pltpu.VMEM((count, len(SHIFTED), rows + 8, LANES), f32)


def tile_at(index):
    return pl.ds(pl.multiple_of(index * LANES, LANES), LANES)


def rows_of(group):
    return slice(group * 8, group * 8 + 8)


def moments_body(load, inv, groups, total_ref, crr_ref, stage_ref):
    row = lax.broadcasted_iota(jnp.int32, (8, LANES), 0)

    def tile(index, _):
        cols = tile_at(index)
        first, second = Window(stage_ref.at[0], row), Window(stage_ref.at[1], row)
        for group in range(groups):
            ret = load(group, cols)
            total, squares = first.push(ret), second.push(ret * ret)
            if group >= W // 8:
                here = rows_of(group - W // 8)
                scale = inv(group - W // 8)
                mean = total * scale
                total_ref[here, cols] = total
                crr_ref[here, cols] = (1.0 - shrink_weight) * (squares * scale - mean * mean)
        return 0

    lax.fori_loop(0, total_ref.shape[1] // LANES, tile, 0)


def moments_main_kernel(ret_ref, mean_ref, crr_ref, stage_ref):
    moments_body(
        lambda group, cols: ret_ref[rows_of(group), cols],
        lambda group: 1.0 / W,
        ret_ref.shape[0] // 8,
        mean_ref,
        crr_ref,
        stage_ref,
    )


def moments_head_kernel(inv_ref, halo_ref, ret_ref, mean_ref, crr_ref, stage_ref):
    blocks = W // 8
    moments_body(
        lambda group, cols: halo_ref[rows_of(group), cols] * inv_ref[W:]
        if group < blocks
        else ret_ref[rows_of(group - blocks), cols],
        lambda group: inv_ref[rows_of(group)],
        2 * blocks,
        mean_ref,
        crr_ref,
        stage_ref,
    )


def sector_rows(means, inv, groups, starts, left_ref, stage_ref, out, low, kept=None):
    row = lax.broadcasted_iota(jnp.int32, (8, LANES), 0)
    spot = 2 * (out // LANES) % stage_ref.shape[0]
    first, second = Window(stage_ref.at[spot], row), Window(stage_ref.at[spot + 1], row)
    mean_parts, gain_parts = [], []
    for group in range(groups):
        mean = means[group]
        total, squares = first.push(mean), second.push(mean * mean)
        if group >= W // 8:
            scale = inv(group - W // 8)
            mean_f = total * scale
            spread = squares * scale - mean_f * mean_f + ridge_rate
            mean_parts.append(mean_f)
            gain_parts.append((1.0 - shrink_weight) * scale * scale / spread)
    for start, parts in zip(starts, (means[:kept], mean_parts, gain_parts)):
        for pair in range(0, len(parts), 2):
            hi, lo = split2(jnp.concatenate(parts[pair : pair + 2], axis=0))
            here = slice(start + pair * 8, start + pair * 8 + 16)
            left_ref[here, out : out + LANES] = hi
            left_ref[here, out + low : out + low + LANES] = lo


def pipelined(fill, work, buffers, chunks):
    even, odd = buffers
    fill(even, 0)

    def pair(j, _):
        fill(odd, 2 * j + 1)
        work(even, 2 * j)
        fill(even, 2 * j + 2)
        work(odd, 2 * j + 1)
        return 0

    lax.fori_loop(0, chunks // 2 - 1, pair, 0)
    fill(odd, chunks - 1)
    work(even, chunks - 2)
    work(odd, chunks - 1)


def chunk_at(index, wide):
    return pl.ds(pl.multiple_of(index * wide, wide), wide)


def main_rows(sums_ref, tail_ref, left_ref, stage_ref):
    main = sums_ref.shape[0]
    rows = main + W
    for tile in range(HALF // LANES):
        cols = slice(tile * LANES, (tile + 1) * LANES)
        scale = 1.0 / jnp.maximum(tail_ref[W : W + 8, cols], 1.0)
        means = [
            (sums_ref[rows_of(g), cols] if g < main // 8 else tail_ref[rows_of(g - main // 8), cols])
            * scale
            for g in range(rows // 8)
        ]
        sector_rows(
            means, lambda g: 1.0 / W, rows // 8, (0, rows, rows + main), left_ref, stage_ref,
            tile * LANES, HALF
        )


def twice(table):
    return jnp.concatenate([table, table], axis=0)


def own_kernel(own_ref, own_tail_ref, table_ref, spread_ref, left_ref, stage_ref):
    main_rows(own_ref, own_tail_ref, left_ref, stage_ref)
    wide = 4 * LANES
    for index in range(table_ref.shape[1] // wide):
        cols = slice(index * wide, (index + 1) * wide)
        spread_ref[:, cols] = dot_nn(left_ref[...], twice(table_ref[:HALF, cols]))


def main_kernel(
    other_ref, other_tail_ref, spread_ref, ret_ref, total_ref, crr_ref, table_ref,
    var_ref, factor_ref, colsum_ref, left_ref, even_ref, odd_ref, stage_ref,
):
    rows = ret_ref.shape[0]
    main = rows - W
    blocks = W // 8
    main_rows(other_ref, other_tail_ref, left_ref, stage_ref)
    row = lax.broadcasted_iota(jnp.int32, (8, LANES), 0)
    wide = even_ref.shape[1]

    def fill(buffer, index):
        cols = chunk_at(index, wide)
        buffer[...] = spread_ref[:, cols] + dot_nn(left_ref[...], twice(table_ref[HALF:, cols]))

    def work(spread_ref, index):
        for tile in range(wide // LANES):
            inner = slice(tile * LANES, (tile + 1) * LANES)
            cols = pl.ds(pl.multiple_of(index * wide + tile * LANES, LANES), LANES)
            cross = Window(stage_ref.at[tile], row)
            total = jnp.zeros((8, LANES), f32)
            for group in range(rows // 8):
                factor = spread_ref[rows_of(group), inner]
                if group < blocks:
                    factor_ref[rows_of(group), cols] = factor
                product = cross.push(ret_ref[rows_of(group), cols] * factor)
                if group >= blocks:
                    g = group - blocks
                    mean_f = spread_ref[rows_of(rows // 8 + g), inner]
                    gain = spread_ref[rows_of((rows + main) // 8 + g), inner]
                    crf = product - total_ref[rows_of(g), cols] * mean_f
                    variance = crr_ref[rows_of(g), cols] - crf * crf * gain
                    var_ref[rows_of(g), cols] = variance
                    total = total + variance
            colsum_ref[:, cols] = total

    pipelined(fill, work, (even_ref, odd_ref), ret_ref.shape[1] // wide)


def head_kernel(
    inv_ref, flip_ref, own_ref, other_ref, counts_own_ref, counts_other_ref, prior_own_ref, prior_other_ref,
    halo_ref, ret_ref, factor_ref, total_ref, crr_ref, colsum_ref, table_ref,
    var_ref, totals_ref, left_ref, even_ref, odd_ref, acc_ref, stage_ref,
):
    blocks = W // 8
    acc_ref[...] = jnp.zeros_like(acc_ref)
    for tile in range(SECTORS // LANES):
        mine = tile < HALF // LANES
        here, prior, counts = (
            (own_ref, prior_own_ref, counts_own_ref)
            if mine
            else (other_ref, prior_other_ref, counts_other_ref)
        )
        cols = pl.ds((tile * LANES) % HALF, LANES)
        scale = 1.0 / jnp.maximum(counts[W : W + 8, cols], 1.0)
        means = [
            (prior[rows_of(g), cols] * inv_ref[W:] if g < blocks else here[rows_of(g - blocks), cols])
            * scale
            for g in range(2 * blocks)
        ]
        sector_rows(
            means, lambda g: inv_ref[rows_of(g)], 2 * blocks, (0, W, 2 * W), left_ref,
            stage_ref, tile * LANES, SECTORS, blocks,
        )
    row = lax.broadcasted_iota(jnp.int32, (8, LANES), 0)
    wide = even_ref.shape[1]

    def fill(buffer, index):
        cols = chunk_at(index, wide)
        buffer[...] = dot_nn(left_ref[...], twice(table_ref[:, cols]))

    def work(spread_ref, index):
        parts = []
        for tile in range(wide // LANES):
            inner = slice(tile * LANES, (tile + 1) * LANES)
            cols = pl.ds(pl.multiple_of(index * wide + tile * LANES, LANES), LANES)
            cross = Window(stage_ref.at[tile], row)
            total = colsum_ref[:, cols]
            for group in range(2 * blocks):
                g = group - blocks
                if g < 0:
                    product = halo_ref[rows_of(group), cols] * spread_ref[rows_of(group), inner]
                    product = product * inv_ref[W:]
                else:
                    product = ret_ref[rows_of(g), cols] * factor_ref[rows_of(g), cols]
                product = cross.push(product)
                if g >= 0:
                    mean_f = spread_ref[rows_of(blocks + g), inner]
                    gain = spread_ref[rows_of(2 * blocks + g), inner]
                    crf = product - total_ref[rows_of(g), cols] * mean_f
                    variance = crr_ref[rows_of(g), cols] - crf * crf * gain
                    var_ref[rows_of(g), cols] = variance
                    total = total + variance
            hi = total.astype(bf16).astype(f32)
            mid = (total - hi).astype(bf16).astype(f32)
            parts.append(
                jnp.concatenate([hi, mid, total - hi - mid, jnp.zeros_like(hi)], axis=0).astype(bf16)
            )
        acc_ref[...] += dot_nt(
            jnp.concatenate(parts, axis=1), table_ref[:, chunk_at(index, wide)]
        )

    pipelined(fill, work, (even_ref, odd_ref), ret_ref.shape[1] // wide)
    total = jnp.sum(acc_ref[...], axis=0, keepdims=True)
    swapped = jnp.concatenate([total[:, HALF:], total[:, :HALF]], axis=1)
    total = jnp.where(flip_ref[0:1] == 0, total, swapped)
    totals_ref[...] = jnp.broadcast_to(total, totals_ref.shape)


VMEM = pl.BlockSpec(memory_space=pltpu.VMEM)


def kernel_call(body, outs, arrays, scratch=(), flops=0, moved=0):
    return kernel_of(body, outs, arrays, scratch, flops, moved)


def kernel_of(body, outs, arrays, scratch, flops, moved):
    return pl.pallas_call(
        body,
        out_shape=tuple(o if hasattr(o, "dtype") else jax.ShapeDtypeStruct(o, f32) for o in outs),
        in_specs=[VMEM] * len(arrays),
        out_specs=[VMEM] * len(outs),
        scratch_shapes=list(scratch),
        compiler_params=pltpu.CompilerParams(vmem_limit_bytes=10 * MIB),
        cost_estimate=pl.CostEstimate(flops=flops, bytes_accessed=moved, transcendentals=0),
    )(*arrays)


def shrink_kernel(
    all_steps, flip_ref, parts_ref, cown_ref, cother_ref, table_ref, head_ref, main_ref, out_hbm, out_ref, sems
):
    total = jnp.sum(parts_ref[...], axis=0, keepdims=True)
    swapped = jnp.concatenate([total[:, HALF:], total[:, :HALF]], axis=1)
    total = jnp.where(flip_ref[0:1] == 0, total, swapped)
    count = jnp.concatenate([cown_ref[W : W + 1], cother_ref[W : W + 1]], axis=1)
    mean = total / (all_steps * jnp.maximum(count, 1.0))
    left = split3_rows(shrink_weight / (1.0 - shrink_weight) * mean)
    chunks, _, wide = out_ref.shape
    copies = []
    for c in range(chunks):
        cols = slice(c * wide, (c + 1) * wide)
        pooled = jnp.sum(dot_nn(left, table_ref[:, cols]), axis=0, keepdims=True)
        out_ref[c, :W] = head_ref[:, cols] + pooled
        out_ref[c, W:] = main_ref[:, cols] + pooled
        copy = pltpu.make_async_copy(out_ref.at[c], out_hbm.at[:, pl.ds(c * wide, wide)], sems.at[c])
        copy.start()
        copies.append(copy)
    for copy in copies:
        copy.wait()


def shrink(all_steps, flip, parts, own, other, table, head, main):
    width = head.shape[1]
    rows = head.shape[0] + main.shape[0]
    chunks = 4
    return pl.pallas_call(
        functools.partial(shrink_kernel, float(all_steps)),
        out_shape=jax.ShapeDtypeStruct((rows, width), f32),
        in_specs=[VMEM] * 7,
        out_specs=pl.BlockSpec(memory_space=pltpu.HBM),
        scratch_shapes=[
            pltpu.VMEM((chunks, rows, width // chunks), f32),
            pltpu.SemaphoreType.DMA((chunks,)),
        ],
        compiler_params=pltpu.CompilerParams(vmem_limit_bytes=10 * MIB),
        cost_estimate=pl.CostEstimate(
            flops=2 * rows * width, bytes_accessed=8 * rows * width, transcendentals=0
        ),
        name="shrink",
    )(flip, parts, own, other, table, head, main)


def swap(value, axis, bit):
    return lax.ppermute(value, axis, [(i, i ^ bit) for i in range(lax.axis_size(axis))])


def ahead(value, axis):
    count = lax.axis_size(axis)
    return lax.ppermute(value, axis, [(i, (i + 1) % count) for i in range(count)])


def across(value, axis):
    bit = 2
    while bit < lax.axis_size(axis):
        value = value + swap(value, axis, bit)
        bit *= 2
    return value


def step(returns, sector):
    rows, width = returns.shape
    main = rows - W
    n_time, n_series = lax.axis_size("tm"), lax.axis_size("series")
    core = (lax.axis_index("series") % 2).astype(jnp.int32)
    first_step = (lax.axis_index("tm") * rows).astype(jnp.int32)
    wide = 4 * LANES
    hbm = pl.BlockSpec(memory_space=pltpu.HBM)
    keep, send, table, returns, tail, flip, inv = pl.pallas_call(
        load_kernel,
        out_shape=(
            jax.ShapeDtypeStruct((rows + 8, HALF), f32),
            jax.ShapeDtypeStruct((rows + 8, HALF), f32),
            jax.ShapeDtypeStruct((SECTORS, width), bf16),
            jax.ShapeDtypeStruct((rows, width), f32),
            jax.ShapeDtypeStruct((W, width), f32),
            jax.ShapeDtypeStruct((8, SECTORS), jnp.int32),
            jax.ShapeDtypeStruct((W + 8, LANES), f32),
        ),
        in_specs=[hbm, hbm, VMEM, VMEM],
        out_specs=[VMEM] * 7,
        scratch_shapes=[
            pltpu.VMEM((1, width), jnp.int32),
            pltpu.VMEM((2 * rows + 32, wide), bf16),
            pltpu.VMEM((rows + 8, SECTORS), f32),
            pltpu.SemaphoreType.DMA,
            pltpu.SemaphoreType.DMA,
            pltpu.SemaphoreType.DMA((width // wide,)),
        ],
        compiler_params=pltpu.CompilerParams(vmem_limit_bytes=48 * MIB),
        name="load",
    )(
        returns,
        sector[None, :],
        jnp.broadcast_to(core, (8, LANES)),
        jnp.broadcast_to(first_step, (8, LANES)),
    )
    halo = ahead(tail, "tm")
    swapped = swap(send, "series", 1)
    own_tail = across(keep[main:] + swapped[main:], "series")
    own = across(keep[:main] + swapped[:main], "series")
    prior_own = ahead(own_tail[:W], "tm")
    other_tail = swap(own_tail, "series", 1)
    other = swap(own, "series", 1)
    prior_other = swap(prior_own, "series", 1)
    chunk = 4 * LANES
    lhs = 3 * rows - 2 * W
    mean, crr = kernel_call(
        moments_main_kernel, [(main, width)] * 2, [returns], scratch=[stage(2, rows)],
        flops=40 * main * width, moved=12 * main * width,
    )
    mean_head, crr_head = kernel_call(
        moments_head_kernel, [(W, width)] * 2, [inv, halo, returns], scratch=[stage(2, 2 * W)],
        flops=40 * W * width, moved=12 * W * width,
    )
    left = [pltpu.VMEM((lhs, SECTORS), bf16)]
    (spread,) = kernel_call(
        own_kernel, [(lhs, width)], [own, own_tail, table], scratch=left + [stage(4, rows)],
        flops=2 * lhs * width * SECTORS, moved=4 * lhs * width,
    )
    var, factor, colsum = kernel_call(
        main_kernel, [(main, width), (W, width), (8, width)],
        [other, other_tail, spread, returns, mean, crr, table],
        scratch=left + [pltpu.VMEM((lhs, chunk), f32)] * 2 + [stage(4, rows)],
        flops=4 * lhs * width * SECTORS, moved=12 * rows * width,
    )
    var_head, totals = kernel_call(
        head_kernel, [(W, width), (n_time * n_series, SECTORS)],
        [inv, flip, own, other, own_tail, other_tail, prior_own, prior_other, halo, returns, factor,
         mean_head, crr_head, colsum, table],
        scratch=[pltpu.VMEM((3 * W, 2 * SECTORS), bf16)]
        + [pltpu.VMEM((3 * W, chunk), f32)] * 2
        + [pltpu.VMEM((32, SECTORS), f32), stage(8, 2 * W)],
        flops=16 * W * width * SECTORS, moved=12 * W * width,
    )
    parts = lax.all_to_all(totals, ("tm", "series"), 0, 0)
    return shrink(n_time * rows, flip, parts, own_tail, other_tail, table, var_head, var)


def solution(mesh):
    placed = (P("tm", "series"), P("series"))
    return jax.shard_map(step, mesh=mesh, in_specs=placed, out_specs=P("tm", "series"), check_vma=False)
```

```python
import functools

import jax
import jax.numpy as jnp
from jax import lax
from jax.experimental import pallas as pl
from jax.experimental.pallas import tpu as pltpu
from jax.sharding import PartitionSpec as P


W = 64
SECTORS = 512
HALF = SECTORS // 2
LANES = 128

ridge_rate = 0.05
shrink_weight = 0.3

f32 = jnp.float32
bf16 = jnp.bfloat16
MIB = 1024 * 1024


def dot_nn(a, b):
    return lax.dot_general(a, b, (((1,), (0,)), ((), ())), preferred_element_type=f32)


def dot_nt(a, b):
    return lax.dot_general(a, b, (((1,), (1,)), ((), ())), preferred_element_type=f32)


def split2(x):
    hi = x.astype(bf16)
    return hi, (x - hi.astype(f32)).astype(bf16)


def split3_rows(x):
    hi = x.astype(bf16).astype(f32)
    rest = x - hi
    mid = rest.astype(bf16).astype(f32)
    low = rest - mid
    row = lax.broadcasted_iota(jnp.int32, (16, x.shape[1]), 0)
    return jnp.where(row == 0, hi, jnp.where(row == 1, mid, jnp.where(row == 2, low, 0.0))).astype(bf16)


def load_kernel(
    ret_hbm, sec_hbm, core_ref, first_ref,
    keep_ref, send_ref, table_ref, ret_ref, tail_ref, flip_ref, inv_ref,
    sec_ref, left_ref, acc_ref, sec_sem, tail_sem, ret_sems,
):
    rows, width = ret_ref.shape
    wide = left_ref.shape[1]
    height = rows + 16
    chunks = width // wide
    sec_copy = pltpu.make_async_copy(sec_hbm, sec_ref, sec_sem)
    sec_copy.start()
    copies = []
    for c in range(chunks):
        cols = pl.ds(c * wide, wide)
        copy = pltpu.make_async_copy(ret_hbm.at[:, cols], ret_ref.at[:, cols], ret_sems.at[c])
        copy.start()
        copies.append(copy)
    tail_copy = pltpu.make_async_copy(ret_hbm.at[pl.ds(rows - W, W)], tail_ref, tail_sem)
    tail_copy.start()
    flip_ref[...] = jnp.concatenate([core_ref[...]] * (SECTORS // LANES), axis=1)
    position = lax.broadcasted_iota(jnp.int32, (W, LANES), 0) + (first_ref[0:1] + 1)
    inv_ref[:W] = 1.0 / jnp.minimum(position, W).astype(f32)
    inv_ref[W:] = jnp.where(first_ref[...] > 0, 1.0, 0.0)
    left_ref[rows:height] = jnp.ones((16, wide), bf16)
    left_ref[height + rows :] = jnp.zeros((16, wide), bf16)
    turn = jnp.concatenate([core_ref[0:1] * HALF] * (wide // LANES), axis=1)
    sec_copy.wait()
    for c in range(chunks):
        cols = slice(c * wide, (c + 1) * wide)
        label = lax.broadcasted_iota(jnp.int32, (SECTORS, wide), 0)
        table_ref[:, cols] = jnp.where(label == (sec_ref[:, cols] ^ turn), 1.0, 0.0).astype(bf16)
    for c in range(chunks):
        cols = slice(c * wide, (c + 1) * wide)
        copies[c].wait()
        hi, lo = split2(ret_ref[:, cols])
        left_ref[:rows] = hi
        left_ref[height : height + rows] = lo
        part = dot_nt(left_ref[...], table_ref[:, cols])
        part = part[: rows + 8] + part[height : height + rows + 8]
        if c > 0:
            part = acc_ref[...] + part
        if c < chunks - 1:
            acc_ref[...] = part
    keep_ref[...] = part[:, :HALF]
    send_ref[...] = part[:, HALF:]
    tail_copy.wait()


SHIFTED = (1, 2, 4)


class Window:
    def __init__(self, ref, row):
        self.ref, self.row, self.groups = ref, row, 0
        self.rolled = {}
        self.sums = {8: [], 16: [], 32: []}

    def push(self, x):
        here = 8 + 8 * self.groups
        self.groups += 1
        size = 1
        while size < 8:
            if size in SHIFTED:
                slot = SHIFTED.index(size)
                self.ref[slot, here : here + 8] = x
                x = x + self.ref[slot, here - size : here - size + 8]
            else:
                turned = pltpu.roll(x, size, 0)
                before = self.rolled.get(size, turned)
                self.rolled[size] = turned
                x = x + jnp.where(self.row < size, before, turned)
            size *= 2
        while size < W:
            seen = self.sums[size]
            seen.append(x)
            back = size // 8
            if len(seen) <= back:
                return None
            x = x + seen[-1 - back]
            size *= 2
        return x


def stage(count, rows):
    return pltpu.VMEM((count, len(SHIFTED), rows + 8, LANES), f32)


def tile_at(index):
    return pl.ds(pl.multiple_of(index * LANES, LANES), LANES)


def rows_of(group):
    return slice(group * 8, group * 8 + 8)


def moments_body(load, inv, groups, total_ref, crr_ref, stage_ref):
    row = lax.broadcasted_iota(jnp.int32, (8, LANES), 0)

    def tile(index, _):
        cols = tile_at(index)
        first, second = Window(stage_ref.at[0], row), Window(stage_ref.at[1], row)
        for group in range(groups):
            ret = load(group, cols)
            total, squares = first.push(ret), second.push(ret * ret)
            if group >= W // 8:
                here = rows_of(group - W // 8)
                scale = inv(group - W // 8)
                mean = total * scale
                total_ref[here, cols] = total
                crr_ref[here, cols] = (1.0 - shrink_weight) * (squares * scale - mean * mean)
        return 0

    lax.fori_loop(0, total_ref.shape[1] // LANES, tile, 0)


def moments_main_kernel(ret_ref, mean_ref, crr_ref, stage_ref):
    moments_body(
        lambda group, cols: ret_ref[rows_of(group), cols],
        lambda group: 1.0 / W,
        ret_ref.shape[0] // 8,
        mean_ref,
        crr_ref,
        stage_ref,
    )


def moments_head_kernel(inv_ref, halo_ref, ret_ref, mean_ref, crr_ref, stage_ref):
    blocks = W // 8
    moments_body(
        lambda group, cols: halo_ref[rows_of(group), cols] * inv_ref[W:]
        if group < blocks
        else ret_ref[rows_of(group - blocks), cols],
        lambda group: inv_ref[rows_of(group)],
        2 * blocks,
        mean_ref,
        crr_ref,
        stage_ref,
    )


def sector_rows(means, inv, groups, starts, left_ref, stage_ref, out, low, kept=None):
    row = lax.broadcasted_iota(jnp.int32, (8, LANES), 0)
    spot = 2 * (out // LANES) % stage_ref.shape[0]
    first, second = Window(stage_ref.at[spot], row), Window(stage_ref.at[spot + 1], row)
    mean_parts, gain_parts = [], []
    for group in range(groups):
        mean = means[group]
        total, squares = first.push(mean), second.push(mean * mean)
        if group >= W // 8:
            scale = inv(group - W // 8)
            mean_f = total * scale
            spread = squares * scale - mean_f * mean_f + ridge_rate
            mean_parts.append(mean_f)
            gain_parts.append((1.0 - shrink_weight) * scale * scale / spread)
    for start, parts in zip(starts, (means[:kept], mean_parts, gain_parts)):
        for pair in range(0, len(parts), 2):
            hi, lo = split2(jnp.concatenate(parts[pair : pair + 2], axis=0))
            here = slice(start + pair * 8, start + pair * 8 + 16)
            left_ref[here, out : out + LANES] = hi
            left_ref[here, out + low : out + low + LANES] = lo


def pipelined(fill, work, buffers, chunks):
    even, odd = buffers
    fill(even, 0)

    def pair(j, _):
        fill(odd, 2 * j + 1)
        work(even, 2 * j)
        fill(even, 2 * j + 2)
        work(odd, 2 * j + 1)
        return 0

    lax.fori_loop(0, chunks // 2 - 1, pair, 0)
    fill(odd, chunks - 1)
    work(even, chunks - 2)
    work(odd, chunks - 1)


def chunk_at(index, wide):
    return pl.ds(pl.multiple_of(index * wide, wide), wide)


def main_rows(sums_ref, tail_ref, left_ref, stage_ref):
    main = sums_ref.shape[0]
    rows = main + W
    for tile in range(HALF // LANES):
        cols = slice(tile * LANES, (tile + 1) * LANES)
        scale = 1.0 / jnp.maximum(tail_ref[W : W + 8, cols], 1.0)
        means = [
            (sums_ref[rows_of(g), cols] if g < main // 8 else tail_ref[rows_of(g - main // 8), cols])
            * scale
            for g in range(rows // 8)
        ]
        sector_rows(
            means, lambda g: 1.0 / W, rows // 8, (0, rows, rows + main), left_ref, stage_ref,
            tile * LANES, HALF
        )


def twice(table):
    return jnp.concatenate([table, table], axis=0)


def own_kernel(own_ref, own_tail_ref, table_ref, spread_ref, left_ref, stage_ref):
    main_rows(own_ref, own_tail_ref, left_ref, stage_ref)
    wide = 4 * LANES
    for index in range(table_ref.shape[1] // wide):
        cols = slice(index * wide, (index + 1) * wide)
        spread_ref[:, cols] = dot_nn(left_ref[...], twice(table_ref[:HALF, cols]))


def main_kernel(
    other_ref, other_tail_ref, spread_ref, ret_ref, total_ref, crr_ref, table_ref,
    var_ref, factor_ref, colsum_ref, left_ref, even_ref, odd_ref, stage_ref,
):
    rows = ret_ref.shape[0]
    main = rows - W
    blocks = W // 8
    main_rows(other_ref, other_tail_ref, left_ref, stage_ref)
    row = lax.broadcasted_iota(jnp.int32, (8, LANES), 0)
    wide = even_ref.shape[1]

    def fill(buffer, index):
        cols = chunk_at(index, wide)
        buffer[...] = spread_ref[:, cols] + dot_nn(left_ref[...], twice(table_ref[HALF:, cols]))

    def work(spread_ref, index):
        for tile in range(wide // LANES):
            inner = slice(tile * LANES, (tile + 1) * LANES)
            cols = pl.ds(pl.multiple_of(index * wide + tile * LANES, LANES), LANES)
            cross = Window(stage_ref.at[tile], row)
            total = jnp.zeros((8, LANES), f32)
            for group in range(rows // 8):
                factor = spread_ref[rows_of(group), inner]
                if group < blocks:
                    factor_ref[rows_of(group), cols] = factor
                product = cross.push(ret_ref[rows_of(group), cols] * factor)
                if group >= blocks:
                    g = group - blocks
                    mean_f = spread_ref[rows_of(rows // 8 + g), inner]
                    gain = spread_ref[rows_of((rows + main) // 8 + g), inner]
                    crf = product - total_ref[rows_of(g), cols] * mean_f
                    variance = crr_ref[rows_of(g), cols] - crf * crf * gain
                    var_ref[rows_of(g), cols] = variance
                    total = total + variance
            colsum_ref[:, cols] = total

    pipelined(fill, work, (even_ref, odd_ref), ret_ref.shape[1] // wide)


def head_rows(here_ref, prior_ref, counts_ref, inv_ref, left_ref, stage_ref):
    blocks = W // 8
    for tile in range(HALF // LANES):
        cols = slice(tile * LANES, (tile + 1) * LANES)
        scale = 1.0 / jnp.maximum(counts_ref[W : W + 8, cols], 1.0)
        means = [
            (prior_ref[rows_of(g), cols] * inv_ref[W:] if g < blocks else here_ref[rows_of(g - blocks), cols])
            * scale
            for g in range(2 * blocks)
        ]
        sector_rows(
            means, lambda g: inv_ref[rows_of(g)], 2 * blocks, (0, W, 2 * W), left_ref,
            stage_ref, tile * LANES, HALF, blocks,
        )


def head_own_kernel(
    inv_ref, here_ref, prior_ref, counts_ref, table_ref, spread_ref, left_ref, stage_ref
):
    head_rows(here_ref, prior_ref, counts_ref, inv_ref, left_ref, stage_ref)
    wide = 4 * LANES
    for index in range(table_ref.shape[1] // wide):
        cols = slice(index * wide, (index + 1) * wide)
        spread_ref[:, cols] = dot_nn(left_ref[...], twice(table_ref[:HALF, cols]))


def head_kernel(
    inv_ref, flip_ref, here_ref, prior_ref, counts_ref, spread_ref,
    halo_ref, ret_ref, factor_ref, total_ref, crr_ref, colsum_ref, table_ref,
    var_ref, totals_ref, left_ref, even_ref, odd_ref, acc_ref, stage_ref,
):
    blocks = W // 8
    acc_ref[...] = jnp.zeros_like(acc_ref)
    head_rows(here_ref, prior_ref, counts_ref, inv_ref, left_ref, stage_ref)
    row = lax.broadcasted_iota(jnp.int32, (8, LANES), 0)
    wide = even_ref.shape[1]

    def fill(buffer, index):
        cols = chunk_at(index, wide)
        buffer[...] = spread_ref[:, cols] + dot_nn(left_ref[...], twice(table_ref[HALF:, cols]))

    def work(spread_ref, index):
        parts = []
        for tile in range(wide // LANES):
            inner = slice(tile * LANES, (tile + 1) * LANES)
            cols = pl.ds(pl.multiple_of(index * wide + tile * LANES, LANES), LANES)
            cross = Window(stage_ref.at[tile], row)
            total = colsum_ref[:, cols]
            for group in range(2 * blocks):
                g = group - blocks
                if g < 0:
                    product = halo_ref[rows_of(group), cols] * spread_ref[rows_of(group), inner]
                    product = product * inv_ref[W:]
                else:
                    product = ret_ref[rows_of(g), cols] * factor_ref[rows_of(g), cols]
                product = cross.push(product)
                if g >= 0:
                    mean_f = spread_ref[rows_of(blocks + g), inner]
                    gain = spread_ref[rows_of(2 * blocks + g), inner]
                    crf = product - total_ref[rows_of(g), cols] * mean_f
                    variance = crr_ref[rows_of(g), cols] - crf * crf * gain
                    var_ref[rows_of(g), cols] = variance
                    total = total + variance
            hi = total.astype(bf16).astype(f32)
            mid = (total - hi).astype(bf16).astype(f32)
            parts.append(
                jnp.concatenate([hi, mid, total - hi - mid, jnp.zeros_like(hi)], axis=0).astype(bf16)
            )
        acc_ref[...] += dot_nt(
            jnp.concatenate(parts, axis=1), table_ref[:, chunk_at(index, wide)]
        )

    pipelined(fill, work, (even_ref, odd_ref), ret_ref.shape[1] // wide)
    total = jnp.sum(acc_ref[...], axis=0, keepdims=True)
    swapped = jnp.concatenate([total[:, HALF:], total[:, :HALF]], axis=1)
    total = jnp.where(flip_ref[0:1] == 0, total, swapped)
    totals_ref[...] = jnp.broadcast_to(total, totals_ref.shape)


VMEM = pl.BlockSpec(memory_space=pltpu.VMEM)


def kernel_call(body, outs, arrays, scratch=(), flops=0, moved=0):
    return kernel_of(body, outs, arrays, scratch, flops, moved)


def kernel_of(body, outs, arrays, scratch, flops, moved):
    return pl.pallas_call(
        body,
        out_shape=tuple(o if hasattr(o, "dtype") else jax.ShapeDtypeStruct(o, f32) for o in outs),
        in_specs=[VMEM] * len(arrays),
        out_specs=[VMEM] * len(outs),
        scratch_shapes=list(scratch),
        compiler_params=pltpu.CompilerParams(vmem_limit_bytes=10 * MIB),
        cost_estimate=pl.CostEstimate(flops=flops, bytes_accessed=moved, transcendentals=0),
    )(*arrays)


def shrink_kernel(
    all_steps, flip_ref, parts_ref, cown_ref, cother_ref, table_ref, head_ref, main_ref, out_hbm, out_ref, sems
):
    total = jnp.sum(parts_ref[...], axis=0, keepdims=True)
    swapped = jnp.concatenate([total[:, HALF:], total[:, :HALF]], axis=1)
    total = jnp.where(flip_ref[0:1] == 0, total, swapped)
    count = jnp.concatenate([cown_ref[W : W + 1], cother_ref[W : W + 1]], axis=1)
    mean = total / (all_steps * jnp.maximum(count, 1.0))
    left = split3_rows(shrink_weight / (1.0 - shrink_weight) * mean)
    chunks, _, wide = out_ref.shape
    copies = []
    for c in range(chunks):
        cols = slice(c * wide, (c + 1) * wide)
        pooled = jnp.sum(dot_nn(left, table_ref[:, cols]), axis=0, keepdims=True)
        out_ref[c, :W] = head_ref[:, cols] + pooled
        out_ref[c, W:] = main_ref[:, cols] + pooled
        copy = pltpu.make_async_copy(out_ref.at[c], out_hbm.at[:, pl.ds(c * wide, wide)], sems.at[c])
        copy.start()
        copies.append(copy)
    for copy in copies:
        copy.wait()


def shrink(all_steps, flip, parts, own, other, table, head, main):
    width = head.shape[1]
    rows = head.shape[0] + main.shape[0]
    chunks = 8
    return pl.pallas_call(
        functools.partial(shrink_kernel, float(all_steps)),
        out_shape=jax.ShapeDtypeStruct((rows, width), f32),
        in_specs=[VMEM] * 7,
        out_specs=pl.BlockSpec(memory_space=pltpu.HBM),
        scratch_shapes=[
            pltpu.VMEM((chunks, rows, width // chunks), f32),
            pltpu.SemaphoreType.DMA((chunks,)),
        ],
        compiler_params=pltpu.CompilerParams(vmem_limit_bytes=10 * MIB),
        cost_estimate=pl.CostEstimate(
            flops=2 * rows * width, bytes_accessed=8 * rows * width, transcendentals=0
        ),
        name="shrink",
    )(flip, parts, own, other, table, head, main)


def swap(value, axis, bit):
    return lax.ppermute(value, axis, [(i, i ^ bit) for i in range(lax.axis_size(axis))])


def ahead(value, axis):
    count = lax.axis_size(axis)
    return lax.ppermute(value, axis, [(i, (i + 1) % count) for i in range(count)])


def across(value, axis):
    bit = 2
    while bit < lax.axis_size(axis):
        value = value + swap(value, axis, bit)
        bit *= 2
    return value


def step(returns, sector):
    rows, width = returns.shape
    main = rows - W
    n_time, n_series = lax.axis_size("tm"), lax.axis_size("series")
    core = (lax.axis_index("series") % 2).astype(jnp.int32)
    first_step = (lax.axis_index("tm") * rows).astype(jnp.int32)
    wide = 4 * LANES
    hbm = pl.BlockSpec(memory_space=pltpu.HBM)
    keep, send, table, returns, tail, flip, inv = pl.pallas_call(
        load_kernel,
        out_shape=(
            jax.ShapeDtypeStruct((rows + 8, HALF), f32),
            jax.ShapeDtypeStruct((rows + 8, HALF), f32),
            jax.ShapeDtypeStruct((SECTORS, width), bf16),
            jax.ShapeDtypeStruct((rows, width), f32),
            jax.ShapeDtypeStruct((W, width), f32),
            jax.ShapeDtypeStruct((8, SECTORS), jnp.int32),
            jax.ShapeDtypeStruct((W + 8, LANES), f32),
        ),
        in_specs=[hbm, hbm, VMEM, VMEM],
        out_specs=[VMEM] * 7,
        scratch_shapes=[
            pltpu.VMEM((1, width), jnp.int32),
            pltpu.VMEM((2 * rows + 32, wide), bf16),
            pltpu.VMEM((rows + 8, SECTORS), f32),
            pltpu.SemaphoreType.DMA,
            pltpu.SemaphoreType.DMA,
            pltpu.SemaphoreType.DMA((width // wide,)),
        ],
        compiler_params=pltpu.CompilerParams(vmem_limit_bytes=48 * MIB),
        name="load",
    )(
        returns,
        sector[None, :],
        jnp.broadcast_to(core, (8, LANES)),
        jnp.broadcast_to(first_step, (8, LANES)),
    )
    halo = ahead(tail, "tm")
    swapped = swap(send, "series", 1)
    own_tail = across(keep[main:] + swapped[main:], "series")
    own = across(keep[:main] + swapped[:main], "series")
    prior_own = ahead(own_tail[:W], "tm")
    other_tail = swap(own_tail, "series", 1)
    other = swap(own, "series", 1)
    prior_other = swap(prior_own, "series", 1)
    chunk = 4 * LANES
    lhs = 3 * rows - 2 * W
    mean, crr = kernel_call(
        moments_main_kernel, [(main, width)] * 2, [returns], scratch=[stage(2, rows)],
        flops=40 * main * width, moved=12 * main * width,
    )
    mean_head, crr_head = kernel_call(
        moments_head_kernel, [(W, width)] * 2, [inv, halo, returns], scratch=[stage(2, 2 * W)],
        flops=40 * W * width, moved=12 * W * width,
    )
    left = [pltpu.VMEM((lhs, SECTORS), bf16)]
    (spread,) = kernel_call(
        own_kernel, [(lhs, width)], [own, own_tail, table], scratch=left + [stage(4, rows)],
        flops=2 * lhs * width * SECTORS, moved=4 * lhs * width,
    )
    var, factor, colsum = kernel_call(
        main_kernel, [(main, width), (W, width), (8, width)],
        [other, other_tail, spread, returns, mean, crr, table],
        scratch=left + [pltpu.VMEM((lhs, chunk), f32)] * 2 + [stage(4, rows)],
        flops=4 * lhs * width * SECTORS, moved=12 * rows * width,
    )
    left = [pltpu.VMEM((3 * W, SECTORS), bf16)]
    (spread_head,) = kernel_call(
        head_own_kernel, [(3 * W, width)], [inv, own, prior_own, own_tail, table],
        scratch=left + [stage(4, 2 * W)], flops=8 * W * width * SECTORS, moved=12 * W * width,
    )
    var_head, totals = kernel_call(
        head_kernel, [(W, width), (n_time * n_series, SECTORS)],
        [inv, flip, other, prior_other, other_tail, spread_head, halo, returns, factor,
         mean_head, crr_head, colsum, table],
        scratch=left
        + [pltpu.VMEM((3 * W, chunk), f32)] * 2
        + [pltpu.VMEM((32, SECTORS), f32), stage(4, 2 * W)],
        flops=16 * W * width * SECTORS, moved=12 * W * width,
    )
    parts = lax.all_to_all(totals, ("tm", "series"), 0, 0)
    return shrink(n_time * rows, flip, parts, own_tail, other_tail, table, var_head, var)


def solution(mesh):
    placed = (P("tm", "series"), P("series"))
    return jax.shard_map(step, mesh=mesh, in_specs=placed, out_specs=P("tm", "series"), check_vma=False)
```
